32 devices in a mesh: group: 8 (over y, x, core), shard: 4 (over z).
Axes of the slice: x: 2, y: 2, z: 4, core: 2. Of those that a mesh axis runs over, the one named last changes fastest.
Arguments:
- momentum: bfloat16 [8, 7168, 2048], P(None, ('group', 'shard'))
- gradient: bfloat16 [8, 7168, 2048], P(None, ('group', 'shard'))
- q_prev: bfloat16 [8, 3, 2048, 128], P('group', None, 'shard'), may hold values from -6 to 6
- owner_group: int32 [8], replicated, may hold values from 0 to 7, as said below
- group_counts: int32 [8], replicated, may hold values from 0 to 3, as said below
Outputs:
- momentum_next: bfloat16 [8, 7168, 2048], P(None, ('group', 'shard'))
- update: bfloat16 [8, 7168, 2048], P(None, ('group', 'shard'))
- q_next: bfloat16 [8, 3, 2048, 128], P('group', None, 'shard')
The draws below stay inside these ranges and needn't reach their ends.
Inputs may be any that keep to these rules, and one draw needn't show every extreme that they name: `owner_group`: each group owns at most 3 experts and some group owns exactly 3; a group's experts fill its slots 0, 1, ... in increasing expert order. `group_counts`: entry g is the number of experts whose owner_group is g, except for one or two groups that own some experts, where it is one less; it equals 3 for some group that owns 3 experts.
All inputs are finite; a program needn't handle non-finite values.
Results may differ from the reference program's by a relative error of at most 0.0059.
Values may be sent and summed in bfloat16 or wider, within the bound.
No kernel may reach another device: no remote copies, remote signals or barrier semaphores. Data moves between devices by JAX's collectives and lax.ppermute only.
A program may use at most 128 MiB of HBM per device.

```python
import math
import jax
import jax.numpy as jnp
from jax import lax

D = 7168
H = 2048
RANK = 128
EXPERTS = 8
CAP = 3
BLOCK = 224
N_GROUP = 8
N_SHARD = 4


def entry_scales(key):
    rows = jnp.arange(D, dtype=jnp.int32)
    position = (rows // BLOCK % N_SHARD).astype(jnp.float32) / max(N_SHARD - 1, 1)
    rising = jnp.exp(math.log(3.0) * (position - 0.5))
    row_scale = jnp.exp(jax.random.uniform(jax.random.fold_in(key, 21), (EXPERTS, D, 1), jnp.float32, math.log(0.3), math.log(3.0)))
    col_scale = jnp.exp(jax.random.uniform(jax.random.fold_in(key, 22), (EXPERTS, 1, H), jnp.float32, math.log(0.3), math.log(3.0)))
    return row_scale * rising[None, :, None] * col_scale


def shared_part(key):
    left_factor = jax.random.normal(jax.random.fold_in(key, 41), (EXPERTS, D, RANK), jnp.float32)
    right_factor = jax.random.normal(jax.random.fold_in(key, 42), (EXPERTS, RANK, H), jnp.float32)
    return jnp.einsum('edk,ekh->edh', left_factor, right_factor) / math.sqrt(RANK)


def noise_part(key, salt):
    base = jax.random.fold_in(key, salt)
    values = jax.random.normal(base, (EXPERTS, D, H), jnp.float32)
    return values


def entries(key, salt):
    mixed = 0.894 * shared_part(key) + 0.447 * noise_part(key, salt)
    return mixed * entry_scales(key)


def draw_momentum(key, part):
    return entries(key, 31).astype(jnp.bfloat16)


def draw_gradient(key, part):
    return (0.5 * entries(key, 32)).astype(jnp.bfloat16)


def owner_plan(key):
    total_slots = N_GROUP * CAP
    full_group = jax.random.randint(jax.random.fold_in(key, 12), (), 0, N_GROUP)
    slot_ids = jnp.arange(total_slots, dtype=jnp.int32)
    scores = jax.random.randint(jax.random.fold_in(key, 11), (total_slots,), 0, 2 ** 20) * total_slots + slot_ids
    scores = jnp.where(slot_ids // CAP == full_group, scores + 2 ** 30, scores)
    forced_groups = jnp.array([N_GROUP // 2, 0, 3], dtype=jnp.int32)
    forced_slots = forced_groups * CAP
    mandated_reward = jnp.array([2, 1, 0], dtype=jnp.int32)
    mandated_flag = slot_ids[:, None] == forced_slots[None, :]
    mandated_rating = 2 ** 30 + 2 ** 29 + jnp.sum(jnp.where(mandated_flag, mandated_reward[None, :], 0), axis=1)
    scores = jnp.where(jnp.any(mandated_flag, axis=1), mandated_rating, scores).astype(jnp.int32)
    picked_scores, chosen = lax.top_k(scores, EXPERTS)
    chosen_group = (chosen // CAP).astype(jnp.int32)
    shuffle = jax.random.permutation(jax.random.fold_in(key, 13), EXPERTS - 3)
    owner = jnp.concatenate([chosen_group[:3], chosen_group[3:][shuffle]]).astype(jnp.int32)
    group_ids = jnp.arange(N_GROUP, dtype=jnp.int32)
    counts = jnp.sum((owner[None, :] == group_ids[:, None]).astype(jnp.int32), axis=1).astype(jnp.int32)
    holds_forced = jnp.any(group_ids[:, None] == forced_groups[None, :], axis=1)
    eligible = (counts >= 1) & (group_ids != full_group) & jnp.logical_not(holds_forced & (counts < 2))
    group_scores = jax.random.randint(jax.random.fold_in(key, 14), (N_GROUP,), 0, 2 ** 20) * N_GROUP + group_ids
    group_scores = jnp.where(eligible, group_scores + 2 ** 26, group_scores)
    top_scores, picked = lax.top_k(group_scores, 2)
    short = jnp.any(group_ids[:, None] == picked[None, :], axis=1) & eligible
    counts = (counts - short.astype(jnp.int32)).astype(jnp.int32)
    return (owner, counts)


def draw_owner_group(key, part):
    return owner_plan(key)[0]


def draw_group_counts(key, part):
    return owner_plan(key)[1]


def levels(key, dims, split, low, top_value):
    loudness, own = 1.0, jax.random.fold_in(key, 6)
    for axis_at, parts in split:
        heights = jnp.exp(jax.random.uniform(jax.random.fold_in(own, axis_at), (parts,), jnp.float32, low / len(split), top_value / len(split)))
        loudness = loudness * jnp.repeat(heights, dims[axis_at] // parts).reshape([-1 if axis == axis_at else 1 for axis in range(len(dims))])
    return loudness


def gaussian(own_key, shape, deviation, limit, shards=(), kind=jnp.bfloat16):
    gain = levels(own_key, shape, shards, -0.22, 0.18) if shards else 1.0
    values = jax.random.normal(own_key, shape, jnp.float32) * deviation * gain
    return jnp.minimum(jnp.maximum(values, -limit), limit).astype(kind)


def setup_inputs(seed: int = 0) -> dict:
    streams_of = jax.random.split(jax.random.key(seed), 6)
    return {
        "momentum": draw_momentum(jax.random.fold_in(streams_of[5], 71), 0),
        "gradient": draw_gradient(jax.random.fold_in(streams_of[5], 71), 0),
        "q_prev": gaussian(streams_of[2], (N_GROUP, CAP, H, RANK), 1.0, 6.0, ((0, 8), (2, 4))),
        "owner_group": draw_owner_group(jax.random.fold_in(streams_of[5], 71), 0),
        "group_counts": draw_group_counts(jax.random.fold_in(streams_of[5], 71), 0),
    }


stability_offset = 1e-06
momentum_decay = 0.6

def owner_slots(owner_group):
    experts = owner_group.shape[0]
    expert_ids = jnp.arange(experts, dtype=jnp.int32)
    same_owner = owner_group[:, None] == owner_group[None, :]
    earlier = expert_ids[None, :] < expert_ids[:, None]
    return lax.optimization_barrier(jnp.sum((same_owner & earlier).astype(jnp.int32), axis=1)).astype(jnp.int32)

def reference(momentum, gradient, q_prev, owner_group, group_counts):
    slot_of = owner_slots(owner_group)
    keep = slot_of < group_counts[owner_group]
    q_each = q_prev[owner_group, slot_of]
    update_multiplier = math.sqrt(D / RANK)

    def one_expert(items):
        moment_one, grad_one, q_one, keep_one = items
        combined = (moment_one.astype(jnp.float32) + grad_one.astype(jnp.float32)).astype(jnp.bfloat16)
        q_used = jnp.where(keep_one, q_one, jnp.zeros_like(q_one))
        unnormalized_basis = jnp.dot(combined, q_used, preferred_element_type=jnp.float32)
        left_unit = (unnormalized_basis * lax.rsqrt(lax.optimization_barrier(jnp.sum(unnormalized_basis * unnormalized_basis, axis=0)) + stability_offset)[None, :]).astype(jnp.bfloat16)
        right = jnp.dot(combined.T, left_unit, preferred_element_type=jnp.float32)
        q_new = (right * lax.rsqrt(lax.optimization_barrier(jnp.mean(right * right, axis=0)) + stability_offset)[None, :]).astype(jnp.bfloat16)
        update_one = (jnp.dot(left_unit, q_new.T, preferred_element_type=jnp.float32) * update_multiplier).astype(jnp.bfloat16)
        low_rank = jnp.dot(left_unit, right.astype(jnp.bfloat16).T, preferred_element_type=jnp.float32)
        moment_next = (combined.astype(jnp.float32) - (1.0 - momentum_decay) * low_rank).astype(jnp.bfloat16)
        return (moment_next, update_one, jnp.where(keep_one, q_new, jnp.zeros_like(q_new)))
    velocity_states, update_list, q_all = lax.map(one_expert, (momentum, gradient, q_each, keep))
    q_next = jnp.zeros_like(q_prev).at[owner_group, slot_of].set(q_all)
    return (velocity_states, update_list, q_next)
```

```python
import functools
import math

import jax
import jax.numpy as jnp
from jax import lax
from jax.experimental import pallas as pl
from jax.experimental.pallas import tpu as pltpu
from jax.sharding import PartitionSpec as P

stability_offset = 1e-06
momentum_decay = 0.6
DOWN = 2.0**-64
UP = 2.0**64
AXES = ("group", "shard")


def owner_slots(owner_group):
    experts = owner_group.shape[0]
    expert_ids = jnp.arange(experts, dtype=jnp.int32)
    same_owner = owner_group[:, None] == owner_group[None, :]
    earlier = expert_ids[None, :] < expert_ids[:, None]
    return jnp.sum((same_owner & earlier).astype(jnp.int32), axis=1)


def bits_of(size):
    bits = []
    bit = 1
    while bit < size:
        bits.append(bit)
        bit *= 2
    assert bit == size
    return bits


class Links:
    def __init__(self, groups, shards):
        self.groups, self.shards = groups, shards

    def swap_group(self, x, bit):
        pairs = [
            (g * self.shards + s, (g ^ bit) * self.shards + s)
            for g in range(self.groups)
            for s in range(self.shards)
        ]
        return lax.ppermute(x, AXES, pairs)

    def swap_shard(self, x, bit):
        pairs = [
            (g * self.shards + s, g * self.shards + (s ^ bit))
            for g in range(self.groups)
            for s in range(self.shards)
        ]
        return lax.ppermute(x, AXES, pairs)

    def shift_shard(self, x, step):
        pairs = [
            (g * self.shards + s, g * self.shards + (s + step) % self.shards)
            for g in range(self.groups)
            for s in range(self.shards)
        ]
        return lax.ppermute(x, AXES, pairs)

    def orders(self):
        near, *far = bits_of(self.groups)
        return near, (far, far[::-1])

    def spread(self, halves):
        near, orders = self.orders()
        held = [{0: half} for half in halves]
        for level in range(len(orders[0])):
            for pieces, order in zip(held, orders):
                bit = order[level]
                for r in list(pieces):
                    pieces[r ^ bit] = self.swap_group(pieces[r], bit)
        for pieces in held:
            for r in list(pieces):
                pieces[r ^ near] = self.swap_group(pieces[r], near)
        return held

    def collect(self, held):
        near, orders = self.orders()
        held = [dict(pieces) for pieces in held]

        def fold(pieces, bit):
            for r in [r for r in pieces if r & bit]:
                arrived = self.swap_group(pieces.pop(r), bit)
                kept = pieces[r ^ bit].astype(jnp.float32)
                pieces[r ^ bit] = (kept + arrived.astype(jnp.float32)).astype(arrived.dtype)

        for pieces in held:
            fold(pieces, near)
        for level in reversed(range(len(orders[0]))):
            for pieces, order in zip(held, orders):
                fold(pieces, order[level])
        return [pieces[0] for pieces in held]


def first_body(where, m_ref, g_ref, qa_ref, qb_ref, c_ref, left_ref, sq_ref, ra_ref, rb_ref):
    half = qa_ref.shape[0]
    combined = (m_ref[0].astype(jnp.float32) + g_ref[0].astype(jnp.float32)).astype(jnp.bfloat16)
    c_ref[...] = combined
    left = jnp.dot(combined[:, :half], qa_ref[...], preferred_element_type=jnp.float32)
    left = left + jnp.dot(combined[:, half:], qb_ref[...], preferred_element_type=jnp.float32)
    left_ref[...] = left
    squares = jnp.sum(left * left, axis=0, keepdims=True)
    sq_ref[...] = jnp.broadcast_to(squares, sq_ref.shape)
    small = (left * DOWN).astype(jnp.bfloat16)
    dims = (((0,), (0,)), ((), ()))
    right = lax.dot_general(small, combined, dims, preferred_element_type=jnp.float32)
    right = right.astype(jnp.bfloat16)
    ra_ref[...] = right[:, :half]
    rb_ref[...] = right[:, half:]


def first_call(where, momentum, gradient, qa, qb):
    experts, rows, hidden = momentum.shape
    half, rank = qa.shape
    block = pl.BlockSpec((1, rows, hidden), lambda i, w: (w[0], 0, 0))
    whole = lambda *shape: pl.BlockSpec(shape, lambda i, w: (0,) * len(shape))
    return pl.pallas_call(
        first_body,
        grid_spec=pltpu.PrefetchScalarGridSpec(
            num_scalar_prefetch=1,
            grid=(1,),
            in_specs=[block, block, whole(half, rank), whole(half, rank)],
            out_specs=[
                whole(rows, hidden),
                whole(rows, rank),
                whole(8, rank),
                whole(rank, half),
                whole(rank, half),
            ],
        ),
        out_shape=[
            jax.ShapeDtypeStruct((rows, hidden), jnp.bfloat16),
            jax.ShapeDtypeStruct((rows, rank), jnp.float32),
            jax.ShapeDtypeStruct((8, rank), jnp.float32),
            jax.ShapeDtypeStruct((rank, half), jnp.bfloat16),
            jax.ShapeDtypeStruct((rank, half), jnp.bfloat16),
        ],
        name="first",
    )(where, momentum, gradient, qa, qb)


def last_body(
    multiplier, where, c_ref, left_ref, sq_ref, ra_ref, rb_ref, pa_ref, pb_ref, *rest
):
    mom_ref, upd_ref, q_ref = rest[-3:]
    half = ra_ref.shape[1]
    squares = sq_ref[...]
    n_row = lax.rsqrt(squares[0:1, :] + stability_offset)
    n_col = lax.rsqrt(squares.T[:, 0:1] + stability_offset) * UP
    left = (left_ref[...] * n_row).astype(jnp.bfloat16)
    ra = ra_ref[...].astype(jnp.float32) * n_col
    rb = rb_ref[...].astype(jnp.float32) * n_col
    total = jnp.sum(ra * ra, axis=1, keepdims=True) + jnp.sum(rb * rb, axis=1, keepdims=True)
    scale = lax.rsqrt(total / (2 * half) + stability_offset)
    for part, right in enumerate((ra, rb)):
        cols = slice(part * half, (part + 1) * half)
        low = jnp.dot(left, right.astype(jnp.bfloat16), preferred_element_type=jnp.float32)
        kept = c_ref[:, cols].astype(jnp.float32)
        mom_ref[0, :, cols] = (kept - (1.0 - momentum_decay) * low).astype(jnp.bfloat16)
        q_new = (right * scale).astype(jnp.bfloat16)
        upd = jnp.dot(left, q_new, preferred_element_type=jnp.float32) * multiplier
        upd_ref[0, :, cols] = upd.astype(jnp.bfloat16)
    own = jnp.where(where[2] == 0, pa_ref[...], pb_ref[...])
    own = own.astype(jnp.float32) * n_col * scale
    q_ref[0] = own.T.astype(jnp.bfloat16)


def last_call(where, combined, left, squares, ra, rb, outs, experts, slots, share, multiplier):
    rows, hidden = combined.shape
    rank, half = ra.shape
    block = pl.BlockSpec((1, rows, hidden), lambda i, w: (w[0], 0, 0))
    whole = lambda *shape: pl.BlockSpec(shape, lambda i, w: (0,) * len(shape))
    part = pl.BlockSpec((rank, share), lambda i, w: (0, w[3]))
    anywhere = pl.BlockSpec(memory_space=pl.ANY)
    return pl.pallas_call(
        functools.partial(last_body, multiplier),
        grid_spec=pltpu.PrefetchScalarGridSpec(
            num_scalar_prefetch=1,
            grid=(1,),
            in_specs=[
                whole(rows, hidden),
                whole(rows, rank),
                whole(8, rank),
                whole(rank, half),
                whole(rank, half),
                part,
                part,
            ]
            + [anywhere] * len(outs),
            out_specs=[
                block,
                block,
                pl.BlockSpec((1, share, rank), lambda i, w: (w[1], 0, 0)),
            ],
        ),
        out_shape=[
            jax.ShapeDtypeStruct((experts, rows, hidden), jnp.bfloat16),
            jax.ShapeDtypeStruct((experts, rows, hidden), jnp.bfloat16),
            jax.ShapeDtypeStruct((slots, share, rank), jnp.bfloat16),
        ],
        input_output_aliases={8 + i: 3 - len(outs) + i for i in range(len(outs))},
        name="last",
    )(where, combined, left, squares, ra, rb, ra, rb, *outs)


def shards(momentum, gradient, q_prev, owner_group, group_counts):
    groups = lax.axis_size("group")
    shard_count = lax.axis_size("shard")
    mine = lax.axis_index("group")
    shard = lax.axis_index("shard")
    experts, rows, hidden = momentum.shape
    _, cap, share, rank = q_prev.shape
    assert experts == groups
    half = hidden // 2
    links = Links(groups, shard_count)
    slot_of = owner_slots(owner_group)
    keep = slot_of < group_counts[owner_group]
    owned = keep & (owner_group == mine)

    q_send = jnp.zeros((experts, share, rank), q_prev.dtype)
    for slot in range(cap):
        here = owned & (slot_of == slot)
        q_send = jnp.where(here[:, None, None], q_prev[0, slot][None], q_send)
    q_recv = lax.all_to_all(q_send, "group", split_axis=0, concat_axis=0, tiled=True)
    q_own = lax.dynamic_index_in_dim(q_recv, owner_group[mine], 0, keepdims=False)
    q_full = lax.all_gather(q_own, "shard", axis=0, tiled=True)
    qs = links.spread([q_full[:half], q_full[half:]])

    order = sorted(qs[0])
    per_half = shard_count // 2
    slots = jnp.where(owned, slot_of, cap)
    where = {}
    for r in order:
        expert = mine ^ r
        where[r] = jnp.stack(
            [expert, slots[expert], shard // per_half, shard % per_half]
        ).astype(jnp.int32)

    kept, squares, rights = {}, {}, [{}, {}]
    for r in order:
        c, left, sq, ra, rb = first_call(where[r], momentum, gradient, qs[0][r], qs[1][r])
        kept[r] = (c, left)
        squares[r] = sq[:1]
        rights[0][r], rights[1][r] = ra, rb

    total = jnp.concatenate([squares[r] for r in order], axis=0)
    for bit in bits_of(shard_count):
        total = total + links.swap_shard(total, bit)
    for bit in bits_of(groups):
        arrived = links.swap_group(total, bit)
        arrived = jnp.concatenate([arrived[r ^ bit : (r ^ bit) + 1] for r in order], axis=0)
        total = total + arrived

    right_a, right_b = links.collect(rights)
    piece = rank // shard_count
    both = jnp.concatenate([right_a, right_b], axis=1).reshape(shard_count, piece, hidden)
    mine_sum = lax.dynamic_index_in_dim(both, shard, 0, keepdims=False).astype(jnp.float32)
    for step in range(1, shard_count):
        target = (shard + step) % shard_count
        out = lax.dynamic_index_in_dim(both, target, 0, keepdims=False)
        mine_sum = mine_sum + links.shift_shard(out, step).astype(jnp.float32)
    right_own = lax.all_gather(mine_sum.astype(jnp.bfloat16), "shard", axis=0, tiled=True)
    full = links.spread([right_own[:, :half], right_own[:, half:]])

    multiplier = math.sqrt(rows * groups * shard_count / rank)
    outs = [jnp.zeros((cap + 1, share, rank), jnp.bfloat16)]
    for r in order:
        sq = jnp.broadcast_to(total[r : r + 1], (8, rank))
        c, left = kept[r]
        outs = last_call(
            where[r], c, left, sq, full[0][r], full[1][r], outs, experts, cap + 1, share, multiplier
        )
    momentum_next, update, q_next = outs
    return momentum_next, update, q_next[None, :cap]


def solution(mesh):
    return jax.shard_map(
        shards,
        mesh=mesh,
        in_specs=(
            P(None, ("group", "shard"), None),
            P(None, ("group", "shard"), None),
            P("group", None, "shard", None),
            P(),
            P(),
        ),
        out_specs=(
            P(None, ("group", "shard"), None),
            P(None, ("group", "shard"), None),
            P("group", None, "shard", None),
        ),
        check_vma=False,
    )
```

```python
import functools
import math

import jax
import jax.numpy as jnp
from jax import lax
from jax.experimental import pallas as pl
from jax.experimental.pallas import tpu as pltpu
from jax.sharding import PartitionSpec as P


stability_offset = 1e-06
momentum_decay = 0.6
DOWN = 2.0**-64
UP = 2.0**64
WEIGHT = 8
AXES = ("group", "shard")


def owner_slots(owner_group):
    experts = owner_group.shape[0]
    expert_ids = jnp.arange(experts, dtype=jnp.int32)
    same_owner = owner_group[:, None] == owner_group[None, :]
    earlier = expert_ids[None, :] < expert_ids[:, None]
    return jnp.sum((same_owner & earlier).astype(jnp.int32), axis=1)


def bits_of(size):
    bits = []
    bit = 1
    while bit < size:
        bits.append(bit)
        bit *= 2
    assert bit == size
    return bits


class Links:
    def __init__(self, groups, shards):
        self.groups, self.shards = groups, shards

    def swap_group(self, x, bit):
        pairs = [
            (g * self.shards + s, (g ^ bit) * self.shards + s)
            for g in range(self.groups)
            for s in range(self.shards)
        ]
        return lax.ppermute(x, AXES, pairs)

    def swap_shard(self, x, bit):
        pairs = [
            (g * self.shards + s, g * self.shards + (s ^ bit))
            for g in range(self.groups)
            for s in range(self.shards)
        ]
        return lax.ppermute(x, AXES, pairs)

    def shift_shard(self, x, step):
        pairs = [
            (g * self.shards + s, g * self.shards + (s + step) % self.shards)
            for g in range(self.groups)
            for s in range(self.shards)
        ]
        return lax.ppermute(x, AXES, pairs)

    def orders(self):
        near, *far = bits_of(self.groups)
        return near, (far, far[::-1])

    def levels(self):
        return len(self.orders()[1][0])

    def cross(self, x, level):
        near, orders = self.orders()
        turn = [orders[1 if g & near else 0][level] for g in range(self.groups)]
        pairs = [
            (g * self.shards + s, (g ^ turn[g]) * self.shards + s)
            for g in range(self.groups)
            for s in range(self.shards)
        ]
        return lax.ppermute(x, AXES, pairs)

    def spread(self, own):
        held = {0: own}
        for level in range(self.levels()):
            for name in list(held):
                held[name | 1 << level] = self.cross(held[name], level)
        return held

    def collect(self, held):
        held = {name: list(pieces) for name, pieces in held.items()}
        for level in reversed(range(self.levels())):
            for name in [name for name in held if name >> level & 1]:
                terms = held.pop(name)
                sent = sum(term.astype(jnp.float32) for term in terms).astype(jnp.bfloat16)
                held[name ^ 1 << level].append(self.cross(sent, level))
        return held[0]


def add_body(m_ref, g_ref, c_ref):
    c_ref[...] = (m_ref[...].astype(jnp.float32) + g_ref[...].astype(jnp.float32)).astype(
        jnp.bfloat16
    )


def add_call(momentum, gradient):
    experts, rows, hidden = momentum.shape
    block = pl.BlockSpec((1, rows, hidden), lambda i: (i, 0, 0))
    return pl.pallas_call(
        add_body,
        grid=(experts,),
        in_specs=[block, block],
        out_specs=block,
        out_shape=jax.ShapeDtypeStruct(momentum.shape, jnp.bfloat16),
        cost_estimate=pl.CostEstimate(
            flops=WEIGHT * experts * 2 * rows * hidden * 128,
            bytes_accessed=6 * momentum.size,
            transcendentals=0,
        ),
        name="add",
    )(momentum, gradient)


def split_body(shard_count, where, *refs):
    ins, outs, total_ref = refs[: -shard_count - 1], refs[-shard_count - 1 : -1], refs[-1]
    total = ins[0][...].astype(jnp.float32)
    for ref in ins[1:]:
        total = total + ref[...].astype(jnp.float32)
    total_ref[...] = total
    piece = outs[0].shape[0]
    for step, out in enumerate(outs):
        start = lax.rem(where[2, 0] + step, shard_count) * piece
        out[...] = total_ref[pl.ds(pl.multiple_of(start, piece), piece), :].astype(jnp.bfloat16)


def split_call(where, terms, shard_count):
    rank, hidden = terms[0].shape
    piece = rank // shard_count
    return pl.pallas_call(
        functools.partial(split_body, shard_count),
        grid_spec=pltpu.PrefetchScalarGridSpec(
            num_scalar_prefetch=1,
            grid=(1,),
            in_specs=[fixed((rank, hidden))] * len(terms),
            out_specs=[fixed((piece, hidden))] * shard_count,
            scratch_shapes=[pltpu.VMEM((rank, hidden), jnp.float32)],
        ),
        out_shape=[jax.ShapeDtypeStruct((piece, hidden), jnp.bfloat16)] * shard_count,
        name="split",
    )(where, *terms)


def load(refs, buf, sems):
    step = pl.program_id(0)

    @pl.when(step == 0)
    def _():
        for j, ref in enumerate(refs):
            pltpu.make_async_copy(ref, buf.at[j], sems.at[j]).start()

    for j, ref in enumerate(refs):

        @pl.when(step == j)
        def _():
            pltpu.make_async_copy(ref, buf.at[j], sems.at[j]).wait()

    return buf[step]


def first_body(count, where, c_ref, *refs):
    q_refs, refs = refs[:count], refs[count:]
    left_ref, right_refs, (buf, sems) = refs[0], refs[1:-2], refs[-2:]
    hidden = c_ref.shape[2]
    step = pl.program_id(0)
    combined = c_ref[0]
    q = load(q_refs, buf, sems)
    left = jnp.dot(combined, q, preferred_element_type=jnp.float32)
    left_ref[0] = left
    squares = jnp.sum(left * left, axis=0, keepdims=True)
    squares = jnp.broadcast_to(squares, (squares.shape[1],) * 2).T.astype(jnp.bfloat16)
    small = (left * DOWN).astype(jnp.bfloat16)
    dims = (((0,), (0,)), ((), ()))
    right = lax.dot_general(small, combined, dims, preferred_element_type=jnp.float32)
    right = right.astype(jnp.bfloat16)
    for j in range(count):

        @pl.when(step == j)
        def _():
            right_refs[j][:, :hidden] = right
            right_refs[j][:, hidden:] = squares


def fixed(shape):
    return pl.BlockSpec(shape, lambda i, w: (0,) * len(shape))


def first_call(where, base, combined, qs):
    _, rows, hidden = combined.shape
    count = len(qs)
    _, rank = qs[0].shape
    outs = pl.pallas_call(
        functools.partial(first_body, count),
        grid_spec=pltpu.PrefetchScalarGridSpec(
            num_scalar_prefetch=1,
            grid=(count,),
            in_specs=[pl.BlockSpec((1, rows, hidden), lambda i, w: (w[0, base + i], 0, 0))]
            + [pl.BlockSpec(memory_space=pl.ANY)] * count,
            out_specs=[pl.BlockSpec((1, rows, rank), lambda i, w: (i, 0, 0))]
            + [fixed((rank, hidden + rank))] * count,
            scratch_shapes=[
                pltpu.VMEM((count, hidden, rank), jnp.bfloat16),
                pltpu.SemaphoreType.DMA((count,)),
            ],
        ),
        out_shape=[jax.ShapeDtypeStruct((count, rows, rank), jnp.float32)]
        + [jax.ShapeDtypeStruct((rank, hidden + rank), jnp.bfloat16)] * count,
        cost_estimate=pl.CostEstimate(
            flops=WEIGHT * count * 4 * rows * hidden * rank,
            bytes_accessed=count * 2 * (rows + 2 * rank) * hidden,
            transcendentals=0,
        ),
        name="first",
    )(where, combined, *qs)
    return outs[0], outs[1:]


def last_body(count, multiplier, cap, base, fresh, where, c_ref, left_ref, *refs):
    right_refs, refs = refs[:count], refs[count:]
    mom_ref, upd_ref, q_ref, buf, sems = refs[-5:]
    step = pl.program_id(0)

    @pl.when(step == 0)
    def _():
        if fresh:
            q_ref[...] = jnp.zeros_like(q_ref)
        else:
            q_ref[...] = refs[0][...]

    hidden = c_ref.shape[2]
    arrived = load(right_refs, buf, sems)
    squares = arrived[:, hidden : hidden + 1].astype(jnp.float32)
    n_col = lax.rsqrt(squares + stability_offset)
    n_row = jnp.broadcast_to(n_col, (n_col.shape[0],) * 2).T[0:1, :]
    n_col = n_col * UP
    left = (left_ref[0] * n_row).astype(jnp.bfloat16)
    right = arrived[:, :hidden].astype(jnp.float32) * n_col
    total = jnp.sum(right * right, axis=1, keepdims=True)
    scale = lax.rsqrt(total / right.shape[1] + stability_offset)
    low = jnp.dot(left, right.astype(jnp.bfloat16), preferred_element_type=jnp.float32)
    kept = c_ref[0].astype(jnp.float32)
    mom_ref[0] = (kept - (1.0 - momentum_decay) * low).astype(jnp.bfloat16)
    q_new = (right * scale).astype(jnp.bfloat16)
    upd = jnp.dot(left, q_new, preferred_element_type=jnp.float32) * multiplier
    upd_ref[0] = upd.astype(jnp.bfloat16)
    slot = where[1, base + step]

    @pl.when(slot < cap)
    def _():
        share = q_ref.shape[1]
        start = pl.multiple_of(where[2, 0] * share, share)
        own = buf[step, :, pl.ds(start, share)].astype(jnp.float32) * n_col * scale
        q_ref[slot] = own.T.astype(jnp.bfloat16)


def last_call(where, base, combined, left, rights, outs, cap, share, multiplier):
    experts, rows, hidden = combined.shape
    count = len(rights)
    rank, width = rights[0].shape
    block = pl.BlockSpec((1, rows, hidden), lambda i, w: (w[0, base + i], 0, 0))
    anywhere = pl.BlockSpec(memory_space=pl.ANY)
    extra = [] if outs is None else [outs[2], outs[0], outs[1]]
    return pl.pallas_call(
        functools.partial(last_body, count, multiplier, cap, base, outs is None),
        grid_spec=pltpu.PrefetchScalarGridSpec(
            num_scalar_prefetch=1,
            grid=(count,),
            in_specs=[
                block,
                pl.BlockSpec((1, rows, rank), lambda i, w: (i, 0, 0)),
            ]
            + [pl.BlockSpec(memory_space=pl.ANY)] * count
            + ([] if outs is None else [fixed((cap, share, rank)), anywhere, anywhere]),
            out_specs=[block, block, fixed((cap, share, rank))],
            scratch_shapes=[
                pltpu.VMEM((count, rank, width), jnp.bfloat16),
                pltpu.SemaphoreType.DMA((count,)),
            ],
        ),
        out_shape=[
            jax.ShapeDtypeStruct((experts, rows, hidden), jnp.bfloat16),
            jax.ShapeDtypeStruct((experts, rows, hidden), jnp.bfloat16),
            jax.ShapeDtypeStruct((cap, share, rank), jnp.bfloat16),
        ],
        input_output_aliases={} if outs is None else {4 + count: 0, 5 + count: 1},
        cost_estimate=pl.CostEstimate(
            flops=WEIGHT * count * 4 * rows * hidden * rank,
            bytes_accessed=count * 2 * (3 * rows + 2 * rank) * hidden,
            transcendentals=0,
        ),
        name="last",
    )(where, combined, left, *rights, *extra)


def step(momentum, gradient, q_prev, owner_group, group_counts):
    groups = lax.axis_size("group")
    shard_count = lax.axis_size("shard")
    mine = lax.axis_index("group")
    shard = lax.axis_index("shard")
    experts, rows, _ = momentum.shape
    _, cap, share, rank = q_prev.shape
    assert experts == groups
    links = Links(groups, shard_count)
    near, orders = links.orders()

    names = range(1 << links.levels())
    most = max(name.bit_count() for name in names)
    sets = [[name for name in names if name.bit_count() == n] for n in range(most + 1)]

    def distances(side):
        reach = lambda name, at: sum(bit for i, bit in enumerate(orders[at]) if name >> i & 1)
        return [
            reach(name, side ^ far) ^ (near if far else 0)
            for members in sets
            for far in (0, 1)
            for name in members
        ]

    slot_of = owner_slots(owner_group)
    owned = (slot_of < group_counts[owner_group]) & (owner_group == mine)
    slots = jnp.where(owned, slot_of, cap)
    chosen = mine ^ jnp.where(
        mine & near > 0, jnp.array(distances(1), jnp.int32), jnp.array(distances(0), jnp.int32)
    )
    where = jnp.stack([chosen, slots[chosen], jnp.full_like(chosen, shard)]).astype(jnp.int32)

    uppers = [r for r in range(groups) if not r & near]

    def outgoing(members):
        picked = slots[mine ^ jnp.array(members, jnp.int32)]
        sent = jnp.zeros((len(members), share, rank), q_prev.dtype)
        for slot in range(cap):
            sent = jnp.where((picked == slot)[:, None, None], q_prev[0, slot][None], sent)
        return sent

    arrived = links.swap_group(outgoing([r ^ near for r in uppers]), near)
    kept = outgoing(uppers)
    parts = [kept[i] + arrived[i] for i in range(len(uppers))]
    q_own = parts[0]
    for part, r in zip(parts[1:], uppers[1:]):
        q_own = q_own + links.swap_group(part, r)
    combined = add_call(momentum, gradient)
    q_own, combined = lax.optimization_barrier((q_own, combined))
    q_full = lax.all_gather(q_own, "shard", axis=0, tiled=True)
    qs = links.spread(q_full)
    qs_far = {name: links.swap_group(piece, near) for name, piece in qs.items()}

    lefts, rights, bases = [], {}, []
    base = 0
    for members in sets:
        count = len(members)
        left, outs = first_call(
            where, base, combined, [qs[n] for n in members] + [qs_far[n] for n in members]
        )
        lefts.append(left)
        for j, name in enumerate(members):
            rights[name] = [outs[j], links.swap_group(outs[count + j], near)]
        bases.append(base)
        base += 2 * count

    pieces = split_call(where, links.collect(rights), shard_count)
    mine_sum = pieces[0].astype(jnp.float32)
    for d in range(1, shard_count):
        mine_sum = mine_sum + links.shift_shard(pieces[d], d).astype(jnp.float32)
    right_own = lax.all_gather(mine_sum.astype(jnp.bfloat16), "shard", axis=0, tiled=True)
    full = links.spread(right_own)
    full_far = {name: links.swap_group(piece, near) for name, piece in full.items()}

    multiplier = math.sqrt(rows * groups * shard_count / rank)
    outs = None
    for i, members in enumerate(sets):
        pieces = [full[name] for name in members] + [full_far[name] for name in members]
        outs = last_call(where, bases[i], combined, lefts[i], pieces, outs, cap, share, multiplier)
    momentum_next, update, q_next = outs
    return momentum_next, update, q_next[None]


def solution(mesh):
    return jax.shard_map(
        step,
        mesh=mesh,
        in_specs=(
            P(None, ("group", "shard"), None),
            P(None, ("group", "shard"), None),
            P("group", None, "shard", None),
            P(),
            P(),
        ),
        out_specs=(
            P(None, ("group", "shard"), None),
            P(None, ("group", "shard"), None),
            P("group", None, "shard", None),
        ),
        check_vma=False,
    )
```

```python
import functools
import math

import jax
import jax.numpy as jnp
from jax import lax
from jax.experimental import pallas as pl
from jax.experimental.pallas import tpu as pltpu
from jax.sharding import PartitionSpec as P


stability_offset = 1e-06
momentum_decay = 0.6
DOWN = 2.0**-64
UP = 2.0**64
WEIGHT = 8
GRANT = 28 * 2**20
AXES = ("group", "shard")


def owner_slots(owner_group):
    experts = owner_group.shape[0]
    expert_ids = jnp.arange(experts, dtype=jnp.int32)
    same_owner = owner_group[:, None] == owner_group[None, :]
    earlier = expert_ids[None, :] < expert_ids[:, None]
    return jnp.sum((same_owner & earlier).astype(jnp.int32), axis=1)


def bits_of(size):
    bits = []
    bit = 1
    while bit < size:
        bits.append(bit)
        bit *= 2
    assert bit == size
    return bits


class Links:
    def __init__(self, groups, shards):
        self.groups, self.shards = groups, shards

    def swap_group(self, x, bit):
        pairs = [
            (g * self.shards + s, (g ^ bit) * self.shards + s)
            for g in range(self.groups)
            for s in range(self.shards)
        ]
        return lax.ppermute(x, AXES, pairs)

    def swap_shard(self, x, bit):
        pairs = [
            (g * self.shards + s, g * self.shards + (s ^ bit))
            for g in range(self.groups)
            for s in range(self.shards)
        ]
        return lax.ppermute(x, AXES, pairs)

    def shift_shard(self, x, step):
        pairs = [
            (g * self.shards + s, g * self.shards + (s + step) % self.shards)
            for g in range(self.groups)
            for s in range(self.shards)
        ]
        return lax.ppermute(x, AXES, pairs)

    def orders(self):
        near, *far = bits_of(self.groups)
        return near, (far, far[::-1])

    def levels(self):
        return len(self.orders()[1][0])

    def cross(self, x, level):
        near, orders = self.orders()
        turn = [orders[1 if g & near else 0][level] for g in range(self.groups)]
        pairs = [
            (g * self.shards + s, (g ^ turn[g]) * self.shards + s)
            for g in range(self.groups)
            for s in range(self.shards)
        ]
        return lax.ppermute(x, AXES, pairs)

    def spread(self, own):
        held = {0: own}
        for level in range(self.levels()):
            for name in list(held):
                held[name | 1 << level] = self.cross(held[name], level)
        return held

    def collect(self, held):
        held = {name: list(pieces) for name, pieces in held.items()}
        for level in reversed(range(self.levels())):
            for name in [name for name in held if name >> level & 1]:
                terms = held.pop(name)
                sent = sum(term.astype(jnp.float32) for term in terms).astype(jnp.bfloat16)
                held[name ^ 1 << level].append(self.cross(sent, level))
        return held[0]


def add_body(m_ref, g_ref, c_ref):
    c_ref[...] = (m_ref[...].astype(jnp.float32) + g_ref[...].astype(jnp.float32)).astype(
        jnp.bfloat16
    )


def add_call(momentum, gradient):
    experts, rows, hidden = momentum.shape
    block = pl.BlockSpec((2, rows, hidden), lambda i: (i, 0, 0))
    return pl.pallas_call(
        add_body,
        grid=(experts // 2,),
        in_specs=[block, block],
        out_specs=block,
        out_shape=jax.ShapeDtypeStruct(momentum.shape, jnp.bfloat16),
        cost_estimate=pl.CostEstimate(
            flops=WEIGHT * experts * 2 * rows * hidden * 128,
            bytes_accessed=6 * momentum.size,
            transcendentals=0,
        ),
        compiler_params=pltpu.CompilerParams(vmem_limit_bytes=GRANT),
        name="add",
    )(momentum, gradient)


def split_body(shard_count, where, *refs):
    ins, outs, total_ref = refs[: -shard_count - 1], refs[-shard_count - 1 : -1], refs[-1]
    total = ins[0][...].astype(jnp.float32)
    for ref in ins[1:]:
        total = total + ref[...].astype(jnp.float32)
    total_ref[...] = total
    piece = outs[0].shape[0]
    for step, out in enumerate(outs):
        start = lax.rem(where[2, 0] + step, shard_count) * piece
        out[...] = total_ref[pl.ds(pl.multiple_of(start, piece), piece), :].astype(jnp.bfloat16)


def split_call(where, terms, shard_count):
    rank, hidden = terms[0].shape
    piece = rank // shard_count
    return pl.pallas_call(
        functools.partial(split_body, shard_count),
        grid_spec=pltpu.PrefetchScalarGridSpec(
            num_scalar_prefetch=1,
            grid=(1,),
            in_specs=[pl.BlockSpec(memory_space=pltpu.VMEM)] * len(terms),
            out_specs=[pl.BlockSpec(memory_space=pltpu.VMEM)] * shard_count,
            scratch_shapes=[pltpu.VMEM((rank, hidden), jnp.float32)],
        ),
        out_shape=[jax.ShapeDtypeStruct((piece, hidden), jnp.bfloat16)] * shard_count,
        compiler_params=pltpu.CompilerParams(vmem_limit_bytes=GRANT),
        name="split",
    )(where, *terms)


def pick(refs):
    value = refs[0][...]
    for j in range(1, len(refs)):
        value = jnp.where(pl.program_id(0) == j, refs[j][...], value)
    return value


def first_body(count, where, c_ref, *refs):
    q_refs, refs = refs[:count], refs[count:]
    left_ref, right_refs = refs[0], refs[1:]
    hidden = c_ref.shape[2]
    step = pl.program_id(0)
    combined = c_ref[0]
    q = pick(q_refs)
    left = jnp.dot(combined, q, preferred_element_type=jnp.float32)
    left_ref[0] = left
    squares = jnp.sum(left * left, axis=0, keepdims=True)
    squares = jnp.broadcast_to(squares, (squares.shape[1],) * 2).T.astype(jnp.bfloat16)
    small = (left * DOWN).astype(jnp.bfloat16)
    dims = (((0,), (0,)), ((), ()))
    right = lax.dot_general(small, combined, dims, preferred_element_type=jnp.float32)
    right = right.astype(jnp.bfloat16)
    for j in range(count):

        @pl.when(step == j)
        def _():
            right_refs[j][:, :hidden] = right
            right_refs[j][:, hidden:] = squares


def fixed(shape):
    return pl.BlockSpec(shape, lambda i, w: (0,) * len(shape))


def first_call(where, base, combined, qs):
    _, rows, hidden = combined.shape
    count = len(qs)
    _, rank = qs[0].shape
    outs = pl.pallas_call(
        functools.partial(first_body, count),
        grid_spec=pltpu.PrefetchScalarGridSpec(
            num_scalar_prefetch=1,
            grid=(count,),
            in_specs=[pl.BlockSpec((1, rows, hidden), lambda i, w: (w[0, base + i], 0, 0))]
            + [pl.BlockSpec(memory_space=pltpu.VMEM)] * count,
            out_specs=[pl.BlockSpec((1, rows, rank), lambda i, w: (i, 0, 0))]
            + [pl.BlockSpec(memory_space=pltpu.VMEM)] * count,
        ),
        out_shape=[jax.ShapeDtypeStruct((count, rows, rank), jnp.float32)]
        + [jax.ShapeDtypeStruct((rank, hidden + rank), jnp.bfloat16)] * count,
        cost_estimate=pl.CostEstimate(
            flops=WEIGHT * count * 4 * rows * hidden * rank,
            bytes_accessed=count * 2 * (rows + 2 * rank) * hidden,
            transcendentals=0,
        ),
        compiler_params=pltpu.CompilerParams(vmem_limit_bytes=GRANT),
        name="first",
    )(where, combined, *qs)
    return outs[0], outs[1:]


def last_body(count, multiplier, cap, base, fresh, where, c_ref, left_ref, *refs):
    right_refs, refs = refs[:count], refs[count:]
    mom_ref, upd_ref, q_ref, buf = refs[-4:]
    step = pl.program_id(0)

    @pl.when(step == 0)
    def _():
        if fresh:
            q_ref[...] = jnp.zeros_like(q_ref)
        else:
            q_ref[...] = refs[0][...]

    hidden = c_ref.shape[2]
    arrived = pick(right_refs)
    buf[...] = arrived
    squares = arrived[:, hidden : hidden + 1].astype(jnp.float32)
    n_col = lax.rsqrt(squares + stability_offset)
    n_row = jnp.broadcast_to(n_col, (n_col.shape[0],) * 2).T[0:1, :]
    n_col = n_col * UP
    left = (left_ref[0] * n_row).astype(jnp.bfloat16)
    right = arrived[:, :hidden].astype(jnp.float32) * n_col
    total = jnp.sum(right * right, axis=1, keepdims=True)
    scale = lax.rsqrt(total / right.shape[1] + stability_offset)
    low = jnp.dot(left, right.astype(jnp.bfloat16), preferred_element_type=jnp.float32)
    kept = c_ref[0].astype(jnp.float32)
    mom_ref[0] = (kept - (1.0 - momentum_decay) * low).astype(jnp.bfloat16)
    q_new = (right * scale).astype(jnp.bfloat16)
    upd = jnp.dot(left, q_new, preferred_element_type=jnp.float32) * multiplier
    upd_ref[0] = upd.astype(jnp.bfloat16)
    slot = where[1, base + step]

    @pl.when(slot < cap)
    def _():
        share = q_ref.shape[1]
        start = pl.multiple_of(where[2, 0] * share, share)
        own = buf[:, pl.ds(start, share)].astype(jnp.float32) * n_col * scale
        q_ref[slot] = own.T.astype(jnp.bfloat16)


def last_call(where, base, combined, left, rights, outs, cap, share, multiplier):
    experts, rows, hidden = combined.shape
    count = len(rights)
    rank, width = rights[0].shape
    block = pl.BlockSpec((1, rows, hidden), lambda i, w: (w[0, base + i], 0, 0))
    anywhere = pl.BlockSpec(memory_space=pl.ANY)
    extra = [] if outs is None else [outs[2], outs[0], outs[1]]
    return pl.pallas_call(
        functools.partial(last_body, count, multiplier, cap, base, outs is None),
        grid_spec=pltpu.PrefetchScalarGridSpec(
            num_scalar_prefetch=1,
            grid=(count,),
            in_specs=[
                block,
                pl.BlockSpec((1, rows, rank), lambda i, w: (i, 0, 0)),
            ]
            + [pl.BlockSpec(memory_space=pltpu.VMEM)] * count
            + ([] if outs is None else [fixed((cap, share, rank)), anywhere, anywhere]),
            out_specs=[block, block, fixed((cap, share, rank))],
            scratch_shapes=[pltpu.VMEM((rank, width), jnp.bfloat16)],
        ),
        out_shape=[
            jax.ShapeDtypeStruct((experts, rows, hidden), jnp.bfloat16),
            jax.ShapeDtypeStruct((experts, rows, hidden), jnp.bfloat16),
            jax.ShapeDtypeStruct((cap, share, rank), jnp.bfloat16),
        ],
        input_output_aliases={} if outs is None else {4 + count: 0, 5 + count: 1},
        cost_estimate=pl.CostEstimate(
            flops=WEIGHT * count * 4 * rows * hidden * rank,
            bytes_accessed=count * 2 * (3 * rows + 2 * rank) * hidden,
            transcendentals=0,
        ),
        compiler_params=pltpu.CompilerParams(vmem_limit_bytes=GRANT),
        name="last",
    )(where, combined, left, *rights, *extra)


def step(momentum, gradient, q_prev, owner_group, group_counts):
    groups = lax.axis_size("group")
    shard_count = lax.axis_size("shard")
    mine = lax.axis_index("group")
    shard = lax.axis_index("shard")
    experts, rows, _ = momentum.shape
    _, cap, share, rank = q_prev.shape
    assert experts == groups
    links = Links(groups, shard_count)
    near, orders = links.orders()

    names = range(1 << links.levels())
    most = max(name.bit_count() for name in names)
    sets = [[name for name in names if name.bit_count() == n] for n in range(most + 1)]

    def distances(side):
        reach = lambda name, at: sum(bit for i, bit in enumerate(orders[at]) if name >> i & 1)
        return [
            reach(name, side ^ far) ^ (near if far else 0)
            for members in sets
            for far in (0, 1)
            for name in members
        ]

    slot_of = owner_slots(owner_group)
    owned = (slot_of < group_counts[owner_group]) & (owner_group == mine)
    slots = jnp.where(owned, slot_of, cap)
    chosen = mine ^ jnp.where(
        mine & near > 0, jnp.array(distances(1), jnp.int32), jnp.array(distances(0), jnp.int32)
    )
    where = jnp.stack([chosen, slots[chosen], jnp.full_like(chosen, shard)]).astype(jnp.int32)

    uppers = [r for r in range(groups) if not r & near]

    def outgoing(members):
        picked = slots[mine ^ jnp.array(members, jnp.int32)]
        sent = jnp.zeros((len(members), share, rank), q_prev.dtype)
        for slot in range(cap):
            sent = jnp.where((picked == slot)[:, None, None], q_prev[0, slot][None], sent)
        return sent

    arrived = links.swap_group(outgoing([r ^ near for r in uppers]), near)
    kept = outgoing(uppers)
    parts = [kept[i] + arrived[i] for i in range(len(uppers))]
    q_own = parts[0]
    for part, r in zip(parts[1:], uppers[1:]):
        q_own = q_own + links.swap_group(part, r)
    combined = add_call(momentum, gradient)
    q_own, combined, where = lax.optimization_barrier((q_own, combined, where))
    q_full = lax.all_gather(q_own, "shard", axis=0, tiled=True)
    qs = links.spread(q_full)
    qs_far = {name: links.swap_group(piece, near) for name, piece in qs.items()}

    lefts, rights, bases = [], {}, []
    base = 0
    for members in sets:
        count = len(members)
        left, outs = first_call(
            where, base, combined, [qs[n] for n in members] + [qs_far[n] for n in members]
        )
        lefts.append(left)
        for j, name in enumerate(members):
            rights[name] = [outs[j], links.swap_group(outs[count + j], near)]
        bases.append(base)
        base += 2 * count

    pieces = split_call(where, links.collect(rights), shard_count)
    mine_sum = pieces[0].astype(jnp.float32)
    for d in range(1, shard_count):
        mine_sum = mine_sum + links.shift_shard(pieces[d], d).astype(jnp.float32)
    right_own = lax.all_gather(mine_sum.astype(jnp.bfloat16), "shard", axis=0, tiled=True)
    full = links.spread(right_own)
    full_far = {name: links.swap_group(piece, near) for name, piece in full.items()}

    multiplier = math.sqrt(rows * groups * shard_count / rank)
    outs = None
    for i, members in enumerate(sets):
        pieces = [full[name] for name in members] + [full_far[name] for name in members]
        outs = last_call(where, bases[i], combined, lefts[i], pieces, outs, cap, share, multiplier)
    momentum_next, update, q_next = outs
    return momentum_next, update, q_next[None]


def solution(mesh):
    return jax.shard_map(
        step,
        mesh=mesh,
        in_specs=(
            P(None, ("group", "shard"), None),
            P(None, ("group", "shard"), None),
            P("group", None, "shard", None),
            P(),
            P(),
        ),
        out_specs=(
            P(None, ("group", "shard"), None),
            P(None, ("group", "shard"), None),
            P("group", None, "shard", None),
        ),
        check_vma=False,
    )
```

```python
import functools
import math

import jax
import jax.numpy as jnp
from jax import lax
from jax.experimental import pallas as pl
from jax.experimental.pallas import tpu as pltpu
from jax.sharding import PartitionSpec as P


stability_offset = 1e-06
momentum_decay = 0.6
DOWN = 2.0**-64
UP = 2.0**64
WEIGHT = 8
GRANT = 28 * 2**20
AXES = ("group", "shard")


def bits_of(size):
    bits = []
    bit = 1
    while bit < size:
        bits.append(bit)
        bit *= 2
    assert bit == size
    return bits


class Links:
    def __init__(self, groups, shards):
        self.groups, self.shards = groups, shards

    def swap_group(self, x, bit):
        pairs = [
            (g * self.shards + s, (g ^ bit) * self.shards + s)
            for g in range(self.groups)
            for s in range(self.shards)
        ]
        return lax.ppermute(x, AXES, pairs)

    def swap_shard(self, x, bit):
        pairs = [
            (g * self.shards + s, g * self.shards + (s ^ bit))
            for g in range(self.groups)
            for s in range(self.shards)
        ]
        return lax.ppermute(x, AXES, pairs)

    def gather_shard(self, x):
        pieces = [x]
        for d in range(1, self.shards):
            pieces.append(self.swap_shard(x, d))
        half = self.shards // 2
        return [jnp.concatenate(pieces[i : i + half], axis=0) for i in (0, half)]

    def orders(self):
        near, *far = bits_of(self.groups)
        return near, (far, far[::-1])

    def levels(self):
        return len(self.orders()[1][0])

    def cross(self, x, level):
        near, orders = self.orders()
        turn = [orders[1 if g & near else 0][level] for g in range(self.groups)]
        pairs = [
            (g * self.shards + s, (g ^ turn[g]) * self.shards + s)
            for g in range(self.groups)
            for s in range(self.shards)
        ]
        return lax.ppermute(x, AXES, pairs)

    def spread(self, own):
        held = {0: own}
        for level in range(self.levels()):
            for name in list(held):
                held[name | 1 << level] = self.cross(held[name], level)
        return held

    def collect(self, held, early):
        held = {name: list(terms) for name, terms in held.items()}
        for level in reversed(range(self.levels())):
            for name in [name for name in held if name >> level & 1]:
                terms = held.pop(name)
                if early and level + 1 < self.levels():
                    sent = sum_call(terms)
                else:
                    sent = sum(term.astype(jnp.float32) for term in terms).astype(jnp.bfloat16)
                held[name ^ 1 << level].append(self.cross(sent, level))
        return held[0]


def plan_body(distances, near, uppers, owner_ref, count_ref, q_ref, table_ref, *refs):
    kept_refs, sent_ref, slots_ref = refs[:-2], refs[-2], refs[-1]
    mine, shard = lax.axis_index("group"), lax.axis_index("shard")
    experts, cap = owner_ref.shape[0], q_ref.shape[1]
    owners = [owner_ref[e] for e in range(experts)]
    for e in range(experts):
        slot = jnp.int32(0)
        for other in owners[:e]:
            slot = slot + (other == owners[e]).astype(jnp.int32)
        live = (slot < count_ref[owners[e]]) & (owners[e] == mine)
        slots_ref[e] = jnp.where(live, slot, cap)
    side = (mine & near) > 0
    for i, (zero, one) in enumerate(zip(*distances)):
        chosen = mine ^ jnp.where(side, one, zero)
        table_ref[0, i] = chosen
        table_ref[1, i] = slots_ref[chosen]
        table_ref[2, i] = shard

    def outgoing(r):
        slot = slots_ref[mine ^ r]
        piece = q_ref[0, jnp.minimum(slot, cap - 1)]
        return jnp.where(slot < cap, piece, jnp.zeros_like(piece))

    for i, r in enumerate(uppers):
        sent_ref[i] = outgoing(r ^ near)
        kept_refs[i][...] = outgoing(r)


def plan_call(owner_group, group_counts, q_prev, distances, near, uppers):
    experts = owner_group.shape[0]
    _, _, share, rank = q_prev.shape
    scalars, vector = (pl.BlockSpec(memory_space=m) for m in (pltpu.SMEM, pltpu.VMEM))
    piece = jax.ShapeDtypeStruct((share, rank), q_prev.dtype)
    outs = pl.pallas_call(
        functools.partial(plan_body, distances, near, uppers),
        grid_spec=pltpu.PrefetchScalarGridSpec(
            num_scalar_prefetch=2,
            grid=(1,),
            in_specs=[pl.BlockSpec(q_prev.shape, lambda i, *_: (0,) * 4)],
            out_specs=[scalars] + [vector] * (len(uppers) + 1),
            scratch_shapes=[pltpu.SMEM((experts,), jnp.int32)],
        ),
        out_shape=[jax.ShapeDtypeStruct((3, experts), jnp.int32)]
        + [piece] * len(uppers)
        + [jax.ShapeDtypeStruct((len(uppers), share, rank), q_prev.dtype)],
        compiler_params=pltpu.CompilerParams(vmem_limit_bytes=GRANT),
        name="plan",
    )(owner_group, group_counts, q_prev)
    return outs[0], outs[1:-1], outs[-1]


def add_body(m_ref, g_ref, c_ref):
    c_ref[...] = (m_ref[...].astype(jnp.float32) + g_ref[...].astype(jnp.float32)).astype(
        jnp.bfloat16
    )


def add_call(momentum, gradient):
    experts, rows, hidden = momentum.shape
    block = pl.BlockSpec((2, rows, hidden), lambda i: (i, 0, 0))
    return pl.pallas_call(
        add_body,
        grid=(experts // 2,),
        in_specs=[block, block],
        out_specs=block,
        out_shape=jax.ShapeDtypeStruct(momentum.shape, jnp.bfloat16),
        cost_estimate=pl.CostEstimate(
            flops=WEIGHT * experts * 2 * rows * hidden * 128,
            bytes_accessed=6 * momentum.size,
            transcendentals=0,
        ),
        compiler_params=pltpu.CompilerParams(vmem_limit_bytes=GRANT),
        name="add",
    )(momentum, gradient)


def sum_body(*refs):
    refs[-1][...] = sum(ref[...].astype(jnp.float32) for ref in refs[:-1]).astype(jnp.bfloat16)


def sum_call(terms):
    vector = pl.BlockSpec(memory_space=pltpu.VMEM)
    return pl.pallas_call(
        sum_body,
        in_specs=[vector] * len(terms),
        out_specs=vector,
        out_shape=jax.ShapeDtypeStruct(terms[0].shape, jnp.bfloat16),
        compiler_params=pltpu.CompilerParams(vmem_limit_bytes=GRANT),
        name="sum",
    )(*terms)


def split_body(half, wholes, where, *refs):
    outs, total_ref = refs[wholes:-1], refs[-1]
    rows = slice(half * total_ref.shape[0], (half + 1) * total_ref.shape[0])
    terms = [ref[rows, :] for ref in refs[:2]] + [ref[...] for ref in refs[2:wholes]]
    total_ref[...] = sum(term.astype(jnp.float32) for term in terms)
    piece = outs[0].shape[0]
    for step, out in enumerate(outs):
        start = (where[2, 0] ^ step) * piece
        out[...] = total_ref[pl.ds(pl.multiple_of(start, piece), piece), :].astype(jnp.bfloat16)


def split_call(where, half, own, parts, shard_count):
    rows, hidden = parts[0].shape
    piece = rows // shard_count
    vector = pl.BlockSpec(memory_space=pltpu.VMEM)
    return pl.pallas_call(
        functools.partial(split_body, half, len(own) + len(parts)),
        grid_spec=pltpu.PrefetchScalarGridSpec(
            num_scalar_prefetch=1,
            grid=(1,),
            in_specs=[vector] * (len(own) + len(parts)),
            out_specs=[vector] * shard_count,
            scratch_shapes=[pltpu.VMEM((rows, hidden), jnp.float32)],
        ),
        out_shape=[jax.ShapeDtypeStruct((piece, hidden), jnp.bfloat16)] * shard_count,
        compiler_params=pltpu.CompilerParams(vmem_limit_bytes=GRANT),
        name="split",
    )(where, *own, *parts)


def pick(refs):
    value = refs[0][...]
    for j in range(1, len(refs)):
        value = jnp.where(pl.program_id(0) == j, refs[j][...], value)
    return value


def first_body(count, shard_count, where, c_ref, *refs):
    q_refs, refs = refs[: 2 * count], refs[2 * count :]
    left_ref, right_refs = refs[0], refs[1:]
    hidden = c_ref.shape[2]
    step = pl.program_id(0)
    combined = c_ref[0]
    halves = [pick(q_refs[:count]), pick(q_refs[count:])]
    share = hidden // shard_count
    left = jnp.zeros(left_ref.shape[1:], jnp.float32)
    for d in range(shard_count):
        start = (where[2, 0] ^ d) * share
        columns = c_ref[0, :, pl.ds(pl.multiple_of(start, share), share)]
        half, at = divmod(d, shard_count // 2)
        part = halves[half][at * share : (at + 1) * share]
        left = left + jnp.dot(columns, part, preferred_element_type=jnp.float32)
    left_ref[0] = left
    squares = jnp.sum(left * left, axis=0, keepdims=True)
    squares = jnp.broadcast_to(squares, (squares.shape[1],) * 2).T.astype(jnp.bfloat16)
    small = (left * DOWN).astype(jnp.bfloat16)
    dims = (((0,), (0,)), ((), ()))
    right = lax.dot_general(small, combined, dims, preferred_element_type=jnp.float32)
    right = right.astype(jnp.bfloat16)
    for j in range(count):

        @pl.when(step == j)
        def _():
            right_refs[j][:, :hidden] = right
            right_refs[j][:, hidden:] = squares


def fixed(shape):
    return pl.BlockSpec(shape, lambda i, w: (0,) * len(shape))


def first_call(where, base, combined, qs, shard_count):
    _, rows, hidden = combined.shape
    count = len(qs) // 2
    _, rank = qs[0].shape
    outs = pl.pallas_call(
        functools.partial(first_body, count, shard_count),
        grid_spec=pltpu.PrefetchScalarGridSpec(
            num_scalar_prefetch=1,
            grid=(count,),
            in_specs=[pl.BlockSpec((1, rows, hidden), lambda i, w: (w[0, base + i], 0, 0))]
            + [pl.BlockSpec(memory_space=pltpu.VMEM)] * len(qs),
            out_specs=[pl.BlockSpec((1, rows, rank), lambda i, w: (i, 0, 0))]
            + [pl.BlockSpec(memory_space=pltpu.VMEM)] * count,
        ),
        out_shape=[jax.ShapeDtypeStruct((count, rows, rank), jnp.float32)]
        + [jax.ShapeDtypeStruct((rank, hidden + rank), jnp.bfloat16)] * count,
        cost_estimate=pl.CostEstimate(
            flops=WEIGHT * count * 4 * rows * hidden * rank,
            bytes_accessed=count * 2 * (rows + 2 * rank) * hidden,
            transcendentals=0,
        ),
        compiler_params=pltpu.CompilerParams(vmem_limit_bytes=GRANT),
        name="first",
    )(where, combined, *qs)
    return outs[0], outs[1:]


def last_body(count, multiplier, cap, base, fresh, where, c_ref, left_ref, *refs):
    right_refs, refs = refs[: 2 * count], refs[2 * count :]
    mom_ref, upd_ref, q_ref, buf = refs[-4:]
    step = pl.program_id(0)

    @pl.when(step == 0)
    def _():
        if fresh:
            q_ref[...] = jnp.zeros_like(q_ref)
        else:
            q_ref[...] = refs[0][...]

    hidden = c_ref.shape[2]
    halves = [pick(right_refs[:count]), pick(right_refs[count:])]
    shard_count = hidden // q_ref.shape[1]
    piece = buf.shape[0] // (2 * shard_count)
    for d in range(shard_count):
        start = (where[2, 0] ^ d) * piece
        half, at = divmod(d, shard_count // 2)
        for i in (0, 1):
            rows = halves[half][(2 * at + i) * piece : (2 * at + i + 1) * piece]
            to = pl.multiple_of(start + i * piece * shard_count, piece)
            buf[pl.ds(to, piece), :] = rows.astype(jnp.float32)
    arrived = buf[...]
    squares = arrived[:, hidden : hidden + 1]
    n_col = lax.rsqrt(squares + stability_offset)
    n_row = jnp.broadcast_to(n_col, (n_col.shape[0],) * 2).T[0:1, :]
    n_col = n_col * UP
    left = (left_ref[0] * n_row).astype(jnp.bfloat16)
    right = arrived[:, :hidden] * n_col
    total = jnp.sum(right * right, axis=1, keepdims=True)
    scale = lax.rsqrt(total / right.shape[1] + stability_offset)
    low = jnp.dot(left, right.astype(jnp.bfloat16), preferred_element_type=jnp.float32)
    kept = c_ref[0].astype(jnp.float32)
    mom_ref[0] = (kept - (1.0 - momentum_decay) * low).astype(jnp.bfloat16)
    q_new = (right * scale).astype(jnp.bfloat16)
    upd = jnp.dot(left, q_new, preferred_element_type=jnp.float32) * multiplier
    upd_ref[0] = upd.astype(jnp.bfloat16)
    slot = where[1, base + step]

    @pl.when(slot < cap)
    def _():
        share = q_ref.shape[1]
        start = pl.multiple_of(where[2, 0] * share, share)
        own = buf[:, pl.ds(start, share)] * n_col * scale
        q_ref[slot] = own.T.astype(jnp.bfloat16)


def last_call(where, base, combined, left, rights, outs, cap, share, multiplier):
    experts, rows, hidden = combined.shape
    count = len(rights) // 2
    rank, width = rights[0].shape
    rank *= 2
    block = pl.BlockSpec((1, rows, hidden), lambda i, w: (w[0, base + i], 0, 0))
    anywhere = pl.BlockSpec(memory_space=pl.ANY)
    extra = [] if outs is None else [outs[2], outs[0], outs[1]]
    return pl.pallas_call(
        functools.partial(last_body, count, multiplier, cap, base, outs is None),
        grid_spec=pltpu.PrefetchScalarGridSpec(
            num_scalar_prefetch=1,
            grid=(count,),
            in_specs=[
                block,
                pl.BlockSpec((1, rows, rank), lambda i, w: (i, 0, 0)),
            ]
            + [pl.BlockSpec(memory_space=pltpu.VMEM)] * len(rights)
            + ([] if outs is None else [fixed((cap, share, rank)), anywhere, anywhere]),
            out_specs=[block, block, fixed((cap, share, rank))],
            scratch_shapes=[pltpu.VMEM((rank, width), jnp.float32)],
        ),
        out_shape=[
            jax.ShapeDtypeStruct((experts, rows, hidden), jnp.bfloat16),
            jax.ShapeDtypeStruct((experts, rows, hidden), jnp.bfloat16),
            jax.ShapeDtypeStruct((cap, share, rank), jnp.bfloat16),
        ],
        input_output_aliases={} if outs is None else {4 + 2 * count: 0, 5 + 2 * count: 1},
        cost_estimate=pl.CostEstimate(
            flops=WEIGHT * count * 4 * rows * hidden * rank,
            bytes_accessed=count * 2 * (3 * rows + 2 * rank) * hidden,
            transcendentals=0,
        ),
        compiler_params=pltpu.CompilerParams(vmem_limit_bytes=GRANT),
        name="last",
    )(where, combined, left, *rights, *extra)


def step(momentum, gradient, q_prev, owner_group, group_counts):
    groups = lax.axis_size("group")
    shard_count = lax.axis_size("shard")
    experts, block, _ = momentum.shape
    _, cap, share, rank = q_prev.shape
    assert experts == groups
    links = Links(groups, shard_count)
    near, orders = links.orders()

    names = range(1 << links.levels())
    most = max(name.bit_count() for name in names)
    sets = [[name for name in names if name.bit_count() == n] for n in range(most + 1)]

    def distances(side):
        reach = lambda name, at: sum(bit for i, bit in enumerate(orders[at]) if name >> i & 1)
        return [
            reach(name, side ^ far) ^ (near if far else 0)
            for members in sets
            for far in (0, 1)
            for name in members
        ]

    uppers = [r for r in range(groups) if not r & near]
    where, kept, sent = plan_call(
        owner_group, group_counts, q_prev, (distances(0), distances(1)), near, uppers
    )
    arrived = links.swap_group(sent, near)
    parts = [kept[i] + arrived[i] for i in range(len(uppers))]
    q_own = parts[0]
    for part, r in zip(parts[1:], uppers[1:]):
        q_own = q_own + links.swap_group(part, r)
    combined = add_call(momentum, gradient)
    q_own, combined = lax.optimization_barrier((q_own, combined))
    q_full = links.gather_shard(q_own)
    qs = [links.spread(part) for part in q_full]
    qs_far = [{n: links.swap_group(x, near) for n, x in part.items()} for part in qs]

    lefts, rights, bases = [], {}, []
    base = 0
    for members in sets:
        count = len(members)
        left, outs = first_call(
            where,
            base,
            combined,
            [
                side[half][n] for half in (0, 1) for side in (qs, qs_far) for n in members
            ],
            shard_count,
        )
        lefts.append(left)
        for j, name in enumerate(members):
            rights[name] = [outs[j], links.swap_group(outs[count + j], near)]
        bases.append(base)
        base += 2 * count

    own = rights.pop(0)
    sums = []
    for i in (0, 1):
        rows = slice(i * rank // 2, (i + 1) * rank // 2)
        held = {name: [term[rows] for term in terms] for name, terms in rights.items()}
        parts = links.collect({0: [], **held}, i == 0)
        pieces = split_call(where, i, own, parts, shard_count)
        mine_sum = pieces[0].astype(jnp.float32)
        for d in range(1, shard_count):
            mine_sum = mine_sum + links.swap_shard(pieces[d], d).astype(jnp.float32)
        sums.append(mine_sum)
    mine_sum = jnp.concatenate(sums, axis=0)
    right_own = links.gather_shard(mine_sum.astype(jnp.bfloat16))
    full = [links.spread(part) for part in right_own]
    full_far = [{n: links.swap_group(x, near) for n, x in part.items()} for part in full]

    multiplier = math.sqrt(block * groups * shard_count / rank)
    outs = None
    for i, members in enumerate(sets):
        pieces = [
            side[half][n] for half in (0, 1) for side in (full, full_far) for n in members
        ]
        outs = last_call(where, bases[i], combined, lefts[i], pieces, outs, cap, share, multiplier)
    momentum_next, update, q_next = outs
    return momentum_next, update, q_next[None]


def solution(mesh):
    return jax.shard_map(
        step,
        mesh=mesh,
        in_specs=(
            P(None, ("group", "shard"), None),
            P(None, ("group", "shard"), None),
            P("group", None, "shard", None),
            P(),
            P(),
        ),
        out_specs=(
            P(None, ("group", "shard"), None),
            P(None, ("group", "shard"), None),
            P("group", None, "shard", None),
        ),
        check_vma=False,
    )
```

```python
import functools
import math

import jax
import jax.numpy as jnp
from jax import lax
from jax.experimental import pallas as pl
from jax.experimental.pallas import tpu as pltpu
from jax.sharding import PartitionSpec as P


stability_offset = 1e-06
momentum_decay = 0.6
DOWN = 2.0**-64
UP = 2.0**64
WEIGHT = 8
GRANT = 28 * 2**20
AXES = ("group", "shard")


def bits_of(size):
    bits = []
    bit = 1
    while bit < size:
        bits.append(bit)
        bit *= 2
    assert bit == size
    return bits


class Links:
    def __init__(self, groups, shards):
        self.groups, self.shards = groups, shards

    def swap_group(self, x, bit):
        pairs = [
            (g * self.shards + s, (g ^ bit) * self.shards + s)
            for g in range(self.groups)
            for s in range(self.shards)
        ]
        return lax.ppermute(x, AXES, pairs)

    def swap_shard(self, x, bit):
        pairs = [
            (g * self.shards + s, g * self.shards + (s ^ bit))
            for g in range(self.groups)
            for s in range(self.shards)
        ]
        return lax.ppermute(x, AXES, pairs)

    def gather_shard(self, x):
        pieces = [x]
        for d in range(1, self.shards):
            pieces.append(self.swap_shard(x, d))
        half = self.shards // 2
        return [jnp.concatenate(pieces[i : i + half], axis=0) for i in (0, half)]

    def orders(self):
        near, *far = bits_of(self.groups)
        return near, (far, far[::-1])

    def levels(self):
        return len(self.orders()[1][0])

    def cross(self, x, level):
        near, orders = self.orders()
        turn = [orders[1 if g & near else 0][level] for g in range(self.groups)]
        pairs = [
            (g * self.shards + s, (g ^ turn[g]) * self.shards + s)
            for g in range(self.groups)
            for s in range(self.shards)
        ]
        return lax.ppermute(x, AXES, pairs)

    def spread(self, own):
        held = {0: own}
        for level in range(self.levels()):
            for name in list(held):
                held[name | 1 << level] = self.cross(held[name], level)
        return held

    def collect(self, held, early):
        held = {name: list(terms) for name, terms in held.items()}
        for level in reversed(range(self.levels())):
            for name in [name for name in held if name >> level & 1]:
                terms = held.pop(name)
                if early and level + 1 < self.levels():
                    sent = sum_call(terms)
                else:
                    sent = sum(term.astype(jnp.float32) for term in terms).astype(jnp.bfloat16)
                held[name ^ 1 << level].append(self.cross(sent, level))
        return held[0]


def plan_body(distances, near, uppers, owner_ref, count_ref, q_ref, table_ref, *refs):
    kept_refs, sent_ref, slots_ref = refs[:-2], refs[-2], refs[-1]
    mine, shard = lax.axis_index("group"), lax.axis_index("shard")
    experts, cap = owner_ref.shape[0], q_ref.shape[1]
    owners = [owner_ref[e] for e in range(experts)]
    for e in range(experts):
        slot = jnp.int32(0)
        for other in owners[:e]:
            slot = slot + (other == owners[e]).astype(jnp.int32)
        live = (slot < count_ref[owners[e]]) & (owners[e] == mine)
        slots_ref[e] = jnp.where(live, slot, cap)
    side = (mine & near) > 0
    for i, (zero, one) in enumerate(zip(*distances)):
        chosen = mine ^ jnp.where(side, one, zero)
        table_ref[0, i] = chosen
        table_ref[1, i] = slots_ref[chosen]
        table_ref[2, i] = shard

    def outgoing(r):
        slot = slots_ref[mine ^ r]
        piece = q_ref[0, jnp.minimum(slot, cap - 1)]
        return jnp.where(slot < cap, piece, jnp.zeros_like(piece))

    for i, r in enumerate(uppers):
        sent_ref[i] = outgoing(r ^ near)
        kept_refs[i][...] = outgoing(r)


def plan_call(owner_group, group_counts, q_prev, distances, near, uppers):
    experts = owner_group.shape[0]
    _, _, share, rank = q_prev.shape
    scalars, vector = (pl.BlockSpec(memory_space=m) for m in (pltpu.SMEM, pltpu.VMEM))
    piece = jax.ShapeDtypeStruct((share, rank), q_prev.dtype)
    outs = pl.pallas_call(
        functools.partial(plan_body, distances, near, uppers),
        grid_spec=pltpu.PrefetchScalarGridSpec(
            num_scalar_prefetch=2,
            grid=(1,),
            in_specs=[pl.BlockSpec(q_prev.shape, lambda i, *_: (0,) * 4)],
            out_specs=[scalars] + [vector] * (len(uppers) + 1),
            scratch_shapes=[pltpu.SMEM((experts,), jnp.int32)],
        ),
        out_shape=[jax.ShapeDtypeStruct((3, experts), jnp.int32)]
        + [piece] * len(uppers)
        + [jax.ShapeDtypeStruct((len(uppers), share, rank), q_prev.dtype)],
        compiler_params=pltpu.CompilerParams(vmem_limit_bytes=GRANT),
        name="plan",
    )(owner_group, group_counts, q_prev)
    return outs[0], outs[1:-1], outs[-1]


def add_body(m_ref, g_ref, c_ref):
    c_ref[...] = (m_ref[...].astype(jnp.float32) + g_ref[...].astype(jnp.float32)).astype(
        jnp.bfloat16
    )


def add_call(momentum, gradient):
    experts, rows, hidden = momentum.shape
    block = pl.BlockSpec((2, rows, hidden), lambda i: (i, 0, 0))
    return pl.pallas_call(
        add_body,
        grid=(experts // 2,),
        in_specs=[block, block],
        out_specs=block,
        out_shape=jax.ShapeDtypeStruct(momentum.shape, jnp.bfloat16),
        cost_estimate=pl.CostEstimate(
            flops=WEIGHT * experts * 2 * rows * hidden * 128,
            bytes_accessed=6 * momentum.size,
            transcendentals=0,
        ),
        compiler_params=pltpu.CompilerParams(vmem_limit_bytes=GRANT),
        name="add",
    )(momentum, gradient)


def sum_body(*refs):
    refs[-1][...] = sum(ref[...].astype(jnp.float32) for ref in refs[:-1]).astype(jnp.bfloat16)


def sum_call(terms):
    vector = pl.BlockSpec(memory_space=pltpu.VMEM)
    return pl.pallas_call(
        sum_body,
        in_specs=[vector] * len(terms),
        out_specs=vector,
        out_shape=jax.ShapeDtypeStruct(terms[0].shape, jnp.bfloat16),
        compiler_params=pltpu.CompilerParams(vmem_limit_bytes=GRANT),
        name="sum",
    )(*terms)


def split_body(half, wholes, where, *refs):
    outs, total_ref = refs[wholes:-1], refs[-1]
    rows = slice(half * total_ref.shape[0], (half + 1) * total_ref.shape[0])
    terms = [ref[rows, :] for ref in refs[:2]] + [ref[...] for ref in refs[2:wholes]]
    total_ref[...] = sum(term.astype(jnp.float32) for term in terms)
    piece = outs[0].shape[0]
    for step, out in enumerate(outs):
        start = (where[2, 0] ^ step) * piece
        out[...] = total_ref[pl.ds(pl.multiple_of(start, piece), piece), :].astype(jnp.bfloat16)


def split_call(where, half, own, parts, shard_count):
    rows, hidden = parts[0].shape
    piece = rows // shard_count
    vector = pl.BlockSpec(memory_space=pltpu.VMEM)
    return pl.pallas_call(
        functools.partial(split_body, half, len(own) + len(parts)),
        grid_spec=pltpu.PrefetchScalarGridSpec(
            num_scalar_prefetch=1,
            grid=(1,),
            in_specs=[vector] * (len(own) + len(parts)),
            out_specs=[vector] * shard_count,
            scratch_shapes=[pltpu.VMEM((rows, hidden), jnp.float32)],
        ),
        out_shape=[jax.ShapeDtypeStruct((piece, hidden), jnp.bfloat16)] * shard_count,
        compiler_params=pltpu.CompilerParams(vmem_limit_bytes=GRANT),
        name="split",
    )(where, *own, *parts)


def pick(refs):
    value = refs[0][...]
    for j in range(1, len(refs)):
        value = jnp.where(pl.program_id(0) == j, refs[j][...], value)
    return value


def first_body(count, shard_count, where, c_ref, *refs):
    q_refs, refs = refs[: 2 * count], refs[2 * count :]
    left_ref, right_refs = refs[0], refs[1:]
    hidden = c_ref.shape[2]
    step = pl.program_id(0)
    combined = c_ref[0]
    halves = [pick(q_refs[:count]), pick(q_refs[count:])]
    share = hidden // shard_count
    left = jnp.zeros(left_ref.shape[1:], jnp.float32)
    for d in range(shard_count):
        start = (where[2, 0] ^ d) * share
        columns = c_ref[0, :, pl.ds(pl.multiple_of(start, share), share)]
        half, at = divmod(d, shard_count // 2)
        part = halves[half][at * share : (at + 1) * share]
        left = left + jnp.dot(columns, part, preferred_element_type=jnp.float32)
    left_ref[0] = left
    squares = jnp.sum(left * left, axis=0, keepdims=True)
    squares = jnp.broadcast_to(squares, (squares.shape[1],) * 2).T.astype(jnp.bfloat16)
    small = (left * DOWN).astype(jnp.bfloat16)
    dims = (((0,), (0,)), ((), ()))
    right = lax.dot_general(small, combined, dims, preferred_element_type=jnp.float32)
    right = right.astype(jnp.bfloat16)
    for j in range(count):

        @pl.when(step == j)
        def _():
            right_refs[j][:, :hidden] = right
            right_refs[j][:, hidden:] = squares


def fixed(shape):
    return pl.BlockSpec(shape, lambda i, w: (0,) * len(shape))


def first_call(where, base, combined, qs, shard_count):
    _, rows, hidden = combined.shape
    count = len(qs) // 2
    _, rank = qs[0].shape
    outs = pl.pallas_call(
        functools.partial(first_body, count, shard_count),
        grid_spec=pltpu.PrefetchScalarGridSpec(
            num_scalar_prefetch=1,
            grid=(count,),
            in_specs=[pl.BlockSpec((1, rows, hidden), lambda i, w: (w[0, base + i], 0, 0))]
            + [pl.BlockSpec(memory_space=pltpu.VMEM)] * len(qs),
            out_specs=[pl.BlockSpec((1, rows, rank), lambda i, w: (i, 0, 0))]
            + [pl.BlockSpec(memory_space=pltpu.VMEM)] * count,
        ),
        out_shape=[jax.ShapeDtypeStruct((count, rows, rank), jnp.float32)]
        + [jax.ShapeDtypeStruct((rank, hidden + rank), jnp.bfloat16)] * count,
        cost_estimate=pl.CostEstimate(
            flops=WEIGHT * count * 4 * rows * hidden * rank,
            bytes_accessed=count * 2 * (rows + 2 * rank) * hidden,
            transcendentals=0,
        ),
        compiler_params=pltpu.CompilerParams(vmem_limit_bytes=GRANT),
        name="first",
    )(where, combined, *qs)
    return outs[0], outs[1:]


def last_body(count, multiplier, cap, base, fresh, where, c_ref, *refs):
    left_refs, refs = refs[: count // 2], refs[count // 2 :]
    right_refs, refs = refs[: 2 * count], refs[2 * count :]
    mom_ref, upd_ref, q_ref, buf = refs[-4:]
    step = pl.program_id(0)

    @pl.when(step == 0)
    def _():
        if fresh:
            q_ref[...] = jnp.zeros_like(q_ref)
        else:
            q_ref[...] = refs[0][...]

    hidden = c_ref.shape[2]
    shard_count = hidden // q_ref.shape[1]
    piece = buf.shape[0] // (2 * shard_count)
    for j in range(count):

        @pl.when(step == j)
        def _():
            for d in range(shard_count):
                half, at = divmod(d, shard_count // 2)
                ref = right_refs[half * count + j]
                for i in (0, 1):
                    rows = ref[(2 * at + i) * piece : (2 * at + i + 1) * piece, :]
                    to = ((where[2, 0] ^ d) + i * shard_count) * piece
                    buf[pl.ds(pl.multiple_of(to, piece), piece), :] = rows.astype(jnp.float32)

    arrived = buf[...]
    squares = arrived[:, hidden : hidden + 1]
    n_col = lax.rsqrt(squares + stability_offset)
    n_row = jnp.broadcast_to(n_col, (n_col.shape[0],) * 2).T[0:1, :]
    n_col = n_col * UP
    left = left_refs[0][0]
    for j in range(1, count // 2):
        left = jnp.where(step // 2 == j, left_refs[j][0], left)
    left = (left * n_row).astype(jnp.bfloat16)
    right = jnp.where(n_col > 0.0, arrived[:, :hidden] * n_col, 0.0)
    total = jnp.sum(right * right, axis=1, keepdims=True)
    scale = lax.rsqrt(total / right.shape[1] + stability_offset)
    low = jnp.dot(left, right.astype(jnp.bfloat16), preferred_element_type=jnp.float32)
    kept = c_ref[0].astype(jnp.float32)
    mom_ref[0] = (kept - (1.0 - momentum_decay) * low).astype(jnp.bfloat16)
    q_new = (right * scale).astype(jnp.bfloat16)
    upd = jnp.dot(left, q_new, preferred_element_type=jnp.float32) * multiplier
    upd_ref[0] = upd.astype(jnp.bfloat16)
    slot = where[1, base + step]

    @pl.when(slot < cap)
    def _():
        share = q_ref.shape[1]
        start = pl.multiple_of(where[2, 0] * share, share)
        own = jnp.where(n_col > 0.0, buf[:, pl.ds(start, share)] * n_col, 0.0) * scale
        q_ref[slot] = own.T.astype(jnp.bfloat16)


def last_call(where, base, combined, left, rights, outs, cap, share, multiplier):
    experts, rows, hidden = combined.shape
    count, pairs = len(rights) // 2, len(left)
    rank, width = rights[0].shape
    rank *= 2
    block = pl.BlockSpec((1, rows, hidden), lambda i, w: (w[0, base + i], 0, 0))
    anywhere = pl.BlockSpec(memory_space=pl.ANY)
    extra = [] if outs is None else [outs[2], outs[0], outs[1]]
    return pl.pallas_call(
        functools.partial(last_body, count, multiplier, cap, base, outs is None),
        grid_spec=pltpu.PrefetchScalarGridSpec(
            num_scalar_prefetch=1,
            grid=(count,),
            in_specs=[block]
            + [
                pl.BlockSpec((1, rows, rank), lambda i, w, j=j: (jnp.clip(i - 2 * j, 0, 1), 0, 0))
                for j in range(len(left))
            ]
            + [pl.BlockSpec(memory_space=pltpu.VMEM)] * len(rights)
            + ([] if outs is None else [fixed((cap, share, rank)), anywhere, anywhere]),
            out_specs=[block, block, fixed((cap, share, rank))],
            scratch_shapes=[pltpu.VMEM((rank, width), jnp.float32)],
        ),
        out_shape=[
            jax.ShapeDtypeStruct((experts, rows, hidden), jnp.bfloat16),
            jax.ShapeDtypeStruct((experts, rows, hidden), jnp.bfloat16),
            jax.ShapeDtypeStruct((cap, share, rank), jnp.bfloat16),
        ],
        input_output_aliases={} if outs is None else {3 + pairs + 2 * count: 0, 4 + pairs + 2 * count: 1},
        cost_estimate=pl.CostEstimate(
            flops=WEIGHT * count * 4 * rows * hidden * rank,
            bytes_accessed=count * 2 * (3 * rows + 2 * rank) * hidden,
            transcendentals=0,
        ),
        compiler_params=pltpu.CompilerParams(vmem_limit_bytes=GRANT),
        name="last",
    )(where, combined, *left, *rights, *extra)


def step(momentum, gradient, q_prev, owner_group, group_counts):
    groups = lax.axis_size("group")
    shard_count = lax.axis_size("shard")
    experts, block, _ = momentum.shape
    _, cap, share, rank = q_prev.shape
    assert experts == groups
    links = Links(groups, shard_count)
    near, orders = links.orders()

    names = in_order(links.levels())
    sets = [[n for n in names if n.bit_count() == i] for i in range(links.levels() + 1)]

    def distances(side):
        reach = lambda name, at: sum(bit for i, bit in enumerate(orders[at]) if name >> i & 1)
        return [
            reach(name, side ^ far) ^ (near if far else 0)
            for name in names
            for far in (0, 1)
        ]

    uppers = [r for r in range(groups) if not r & near]
    where, kept, sent = plan_call(
        owner_group, group_counts, q_prev, (distances(0), distances(1)), near, uppers
    )
    arrived = links.swap_group(sent, near)
    parts = [kept[i] + arrived[i] for i in range(len(uppers))]
    q_own = parts[0]
    for part, r in zip(parts[1:], uppers[1:]):
        q_own = q_own + links.swap_group(part, r)
    combined = add_call(momentum, gradient)
    q_own, combined = lax.optimization_barrier((q_own, combined))
    q_full = links.gather_shard(q_own)
    qs = [links.spread(part) for part in q_full]
    qs_far = [{n: links.swap_group(x, near) for n, x in part.items()} for part in qs]

    lefts, rights = {}, {}
    for i, name in enumerate(names):
        pieces = [side[half][name] for half in (0, 1) for side in (qs, qs_far)]
        lefts[name], outs = first_call(where, 2 * i, combined, pieces, shard_count)
        rights[name] = [outs[0], links.swap_group(outs[1], near)]

    own = rights.pop(0)
    sums = []
    for i in (0, 1):
        rows = slice(i * rank // 2, (i + 1) * rank // 2)
        held = {name: [term[rows] for term in terms] for name, terms in rights.items()}
        parts = links.collect({0: [], **held}, i == 0)
        pieces = split_call(where, i, own, parts, shard_count)
        mine_sum = pieces[0].astype(jnp.float32)
        for d in range(1, shard_count):
            mine_sum = mine_sum + links.swap_shard(pieces[d], d).astype(jnp.float32)
        sums.append(mine_sum)
    mine_sum = jnp.concatenate(sums, axis=0)
    right_own = links.gather_shard(mine_sum.astype(jnp.bfloat16))
    full = [links.spread(part) for part in right_own]
    full_far = [{n: links.swap_group(x, near) for n, x in part.items()} for part in full]

    multiplier = math.sqrt(block * groups * shard_count / rank)
    outs = None
    for members in sets:
        pieces = [
            side[half][n] for half in (0, 1) for n in members for side in (full, full_far)
        ]
        base = 2 * names.index(members[0])
        left = [lefts[n] for n in members]
        outs = last_call(
            where, base, combined, left, pieces, outs, cap, share, multiplier
        )
    momentum_next, update, q_next = outs
    return momentum_next, update, q_next[None]


def in_order(levels):
    return sorted(range(1 << levels), key=lambda name: (name.bit_count(), -name))


def solution(mesh):
    return jax.shard_map(
        step,
        mesh=mesh,
        in_specs=(
            P(None, ("group", "shard"), None),
            P(None, ("group", "shard"), None),
            P("group", None, "shard", None),
            P(),
            P(),
        ),
        out_specs=(
            P(None, ("group", "shard"), None),
            P(None, ("group", "shard"), None),
            P("group", None, "shard", None),
        ),
        check_vma=False,
    )
```

```python
import functools
import math

import jax
import jax.numpy as jnp
from jax import lax
from jax.experimental import pallas as pl
from jax.experimental.pallas import tpu as pltpu
from jax.sharding import PartitionSpec as P


stability_offset = 1e-06
momentum_decay = 0.6
DOWN = 2.0**-64
UP = 2.0**64
WEIGHT = 8
GRANT = 28 * 2**20
AXES = ("group", "shard")


def bits_of(size):
    bits = []
    bit = 1
    while bit < size:
        bits.append(bit)
        bit *= 2
    assert bit == size
    return bits


class Links:
    def __init__(self, groups, shards):
        self.groups, self.shards = groups, shards

    def swap_group(self, x, bit):
        pairs = [
            (g * self.shards + s, (g ^ bit) * self.shards + s)
            for g in range(self.groups)
            for s in range(self.shards)
        ]
        return lax.ppermute(x, AXES, pairs)

    def swap_shard(self, x, bit):
        pairs = [
            (g * self.shards + s, g * self.shards + (s ^ bit))
            for g in range(self.groups)
            for s in range(self.shards)
        ]
        return lax.ppermute(x, AXES, pairs)

    def gather_shard(self, x):
        pieces = [x]
        for d in range(1, self.shards):
            pieces.append(self.swap_shard(x, d))
        half = self.shards // 2
        return [jnp.concatenate(pieces[i : i + half], axis=0) for i in (0, half)]

    def orders(self):
        near, *far = bits_of(self.groups)
        return near, (far, far[::-1])

    def levels(self):
        return len(self.orders()[1][0])

    def cross(self, x, level):
        near, orders = self.orders()
        turn = [orders[1 if g & near else 0][level] for g in range(self.groups)]
        pairs = [
            (g * self.shards + s, (g ^ turn[g]) * self.shards + s)
            for g in range(self.groups)
            for s in range(self.shards)
        ]
        return lax.ppermute(x, AXES, pairs)

    def spread(self, own):
        held = {0: own}
        for level in range(self.levels()):
            for name in list(held):
                held[name | 1 << level] = self.cross(held[name], level)
        return held

    def collect(self, held, early):
        held = {name: list(terms) for name, terms in held.items()}
        for level in reversed(range(self.levels())):
            for name in [name for name in held if name >> level & 1]:
                terms = held.pop(name)
                if early and level + 1 < self.levels():
                    sent = sum_call(terms)
                else:
                    sent = sum(term.astype(jnp.float32) for term in terms).astype(jnp.bfloat16)
                held[name ^ 1 << level].append(self.cross(sent, level))
        return held[0]


def plan_body(distances, near, uppers, owner_ref, count_ref, q_ref, table_ref, *refs):
    kept_refs, sent_ref, slots_ref = refs[:-2], refs[-2], refs[-1]
    mine, shard = lax.axis_index("group"), lax.axis_index("shard")
    experts, cap = owner_ref.shape[0], q_ref.shape[1]
    owners = [owner_ref[e] for e in range(experts)]
    for e in range(experts):
        slot = jnp.int32(0)
        for other in owners[:e]:
            slot = slot + (other == owners[e]).astype(jnp.int32)
        live = (slot < count_ref[owners[e]]) & (owners[e] == mine)
        slots_ref[e] = jnp.where(live, slot, cap)
    side = (mine & near) > 0
    for i, (zero, one) in enumerate(zip(*distances)):
        chosen = mine ^ jnp.where(side, one, zero)
        table_ref[0, i] = chosen
        table_ref[1, i] = slots_ref[chosen]
        table_ref[2, i] = shard

    def outgoing(r):
        slot = slots_ref[mine ^ r]
        piece = q_ref[0, jnp.minimum(slot, cap - 1)]
        return jnp.where(slot < cap, piece, jnp.zeros_like(piece))

    for i, r in enumerate(uppers):
        sent_ref[i] = outgoing(r ^ near)
        kept_refs[i][...] = outgoing(r)


def plan_call(owner_group, group_counts, q_prev, distances, near, uppers):
    experts = owner_group.shape[0]
    _, _, share, rank = q_prev.shape
    scalars, vector = (pl.BlockSpec(memory_space=m) for m in (pltpu.SMEM, pltpu.VMEM))
    piece = jax.ShapeDtypeStruct((share, rank), q_prev.dtype)
    outs = pl.pallas_call(
        functools.partial(plan_body, distances, near, uppers),
        grid_spec=pltpu.PrefetchScalarGridSpec(
            num_scalar_prefetch=2,
            grid=(1,),
            in_specs=[pl.BlockSpec(q_prev.shape, lambda i, *_: (0,) * 4)],
            out_specs=[scalars] + [vector] * (len(uppers) + 1),
            scratch_shapes=[pltpu.SMEM((experts,), jnp.int32)],
        ),
        out_shape=[jax.ShapeDtypeStruct((3, experts), jnp.int32)]
        + [piece] * len(uppers)
        + [jax.ShapeDtypeStruct((len(uppers), share, rank), q_prev.dtype)],
        compiler_params=pltpu.CompilerParams(vmem_limit_bytes=GRANT),
        name="plan",
    )(owner_group, group_counts, q_prev)
    return outs[0], outs[1:-1], outs[-1]


def add_body(m_ref, g_ref, c_ref):
    c_ref[...] = (m_ref[...].astype(jnp.float32) + g_ref[...].astype(jnp.float32)).astype(
        jnp.bfloat16
    )


def add_call(momentum, gradient):
    experts, rows, hidden = momentum.shape
    block = pl.BlockSpec((2, rows, hidden), lambda i: (i, 0, 0))
    return pl.pallas_call(
        add_body,
        grid=(experts // 2,),
        in_specs=[block, block],
        out_specs=block,
        out_shape=jax.ShapeDtypeStruct(momentum.shape, jnp.bfloat16),
        cost_estimate=pl.CostEstimate(
            flops=WEIGHT * experts * 2 * rows * hidden * 128,
            bytes_accessed=6 * momentum.size,
            transcendentals=0,
        ),
        compiler_params=pltpu.CompilerParams(vmem_limit_bytes=GRANT),
        name="add",
    )(momentum, gradient)


def sum_body(*refs):
    refs[-1][...] = sum(ref[...].astype(jnp.float32) for ref in refs[:-1]).astype(jnp.bfloat16)


def sum_call(terms):
    vector = pl.BlockSpec(memory_space=pltpu.VMEM)
    return pl.pallas_call(
        sum_body,
        in_specs=[vector] * len(terms),
        out_specs=vector,
        out_shape=jax.ShapeDtypeStruct(terms[0].shape, jnp.bfloat16),
        compiler_params=pltpu.CompilerParams(vmem_limit_bytes=GRANT),
        name="sum",
    )(*terms)


def split_body(half, wholes, where, *refs):
    outs, total_ref = refs[wholes:-1], refs[-1]
    rows = slice(half * total_ref.shape[0], (half + 1) * total_ref.shape[0])
    terms = [ref[rows, :] for ref in refs[:2]] + [ref[...] for ref in refs[2:wholes]]
    total_ref[...] = sum(term.astype(jnp.float32) for term in terms)
    piece = outs[0].shape[0]
    for step, out in enumerate(outs):
        start = (where[2, 0] ^ step) * piece
        out[...] = total_ref[pl.ds(pl.multiple_of(start, piece), piece), :].astype(jnp.bfloat16)


def split_call(where, half, own, parts, shard_count):
    rows, hidden = parts[0].shape
    piece = rows // shard_count
    vector = pl.BlockSpec(memory_space=pltpu.VMEM)
    return pl.pallas_call(
        functools.partial(split_body, half, len(own) + len(parts)),
        grid_spec=pltpu.PrefetchScalarGridSpec(
            num_scalar_prefetch=1,
            grid=(1,),
            in_specs=[vector] * (len(own) + len(parts)),
            out_specs=[vector] * shard_count,
            scratch_shapes=[pltpu.VMEM((rows, hidden), jnp.float32)],
        ),
        out_shape=[jax.ShapeDtypeStruct((piece, hidden), jnp.bfloat16)] * shard_count,
        compiler_params=pltpu.CompilerParams(vmem_limit_bytes=GRANT),
        name="split",
    )(where, *own, *parts)


def pick(refs):
    value = refs[0][...]
    for j in range(1, len(refs)):
        value = jnp.where(pl.program_id(0) == j, refs[j][...], value)
    return value


def first_body(count, shard_count, where, c_ref, *refs):
    q_refs, refs = refs[: 2 * count], refs[2 * count :]
    left_ref, right_refs = refs[0], refs[1:]
    hidden = c_ref.shape[2]
    step = pl.program_id(0)
    combined = c_ref[0]
    halves = [pick(q_refs[:count]), pick(q_refs[count:])]
    share = hidden // shard_count
    left = jnp.zeros(left_ref.shape[1:], jnp.float32)
    for d in range(shard_count):
        start = (where[2, 0] ^ d) * share
        columns = c_ref[0, :, pl.ds(pl.multiple_of(start, share), share)]
        half, at = divmod(d, shard_count // 2)
        part = halves[half][at * share : (at + 1) * share]
        left = left + jnp.dot(columns, part, preferred_element_type=jnp.float32)
    left_ref[0] = left
    squares = jnp.sum(left * left, axis=0, keepdims=True)
    squares = jnp.broadcast_to(squares, (squares.shape[1],) * 2).T.astype(jnp.bfloat16)
    small = (left * DOWN).astype(jnp.bfloat16)
    dims = (((0,), (0,)), ((), ()))
    right = lax.dot_general(small, combined, dims, preferred_element_type=jnp.float32)
    right = right.astype(jnp.bfloat16)
    for j in range(count):

        @pl.when(step == j)
        def _():
            right_refs[j][:, :hidden] = right
            right_refs[j][:, hidden:] = squares


def fixed(shape):
    return pl.BlockSpec(shape, lambda i, w: (0,) * len(shape))


def first_call(where, base, combined, qs, shard_count):
    _, rows, hidden = combined.shape
    count = len(qs) // 2
    _, rank = qs[0].shape
    outs = pl.pallas_call(
        functools.partial(first_body, count, shard_count),
        grid_spec=pltpu.PrefetchScalarGridSpec(
            num_scalar_prefetch=1,
            grid=(count,),
            in_specs=[pl.BlockSpec((1, rows, hidden), lambda i, w: (w[0, base + i], 0, 0))]
            + [pl.BlockSpec(memory_space=pltpu.VMEM)] * len(qs),
            out_specs=[pl.BlockSpec((1, rows, rank), lambda i, w: (i, 0, 0))]
            + [pl.BlockSpec(memory_space=pltpu.VMEM)] * count,
        ),
        out_shape=[jax.ShapeDtypeStruct((count, rows, rank), jnp.float32)]
        + [jax.ShapeDtypeStruct((rank, hidden + rank), jnp.bfloat16)] * count,
        cost_estimate=pl.CostEstimate(
            flops=WEIGHT * count * 4 * rows * hidden * rank,
            bytes_accessed=count * 2 * (rows + 2 * rank) * hidden,
            transcendentals=0,
        ),
        compiler_params=pltpu.CompilerParams(vmem_limit_bytes=GRANT),
        name="first",
    )(where, combined, *qs)
    return outs[0], outs[1:]


def last_body(count, multiplier, cap, base, fresh, where, c_ref, *refs):
    left_refs, refs = refs[: count // 2], refs[count // 2 :]
    right_refs, refs = refs[: 2 * count], refs[2 * count :]
    mom_ref, upd_ref, q_ref, buf = refs[-4:]
    step = pl.program_id(0)

    @pl.when(step == 0)
    def _():
        if fresh:
            q_ref[...] = jnp.zeros_like(q_ref)
        else:
            q_ref[...] = refs[0][...]

    hidden = c_ref.shape[2]
    shard_count = hidden // q_ref.shape[1]
    piece = buf.shape[0] // (2 * shard_count)
    for j in range(count):

        @pl.when(step == j)
        def _():
            for d in range(shard_count):
                half, at = divmod(d, shard_count // 2)
                ref = right_refs[half * count + j]
                for i in (0, 1):
                    rows = ref[(2 * at + i) * piece : (2 * at + i + 1) * piece, :]
                    to = ((where[2, 0] ^ d) + i * shard_count) * piece
                    buf[pl.ds(pl.multiple_of(to, piece), piece), :] = rows.astype(jnp.float32)

    arrived = buf[...]
    squares = arrived[:, hidden : hidden + 1]
    n_col = lax.rsqrt(squares + stability_offset)
    n_row = jnp.broadcast_to(n_col, (n_col.shape[0],) * 2).T[0:1, :]
    n_col = n_col * UP
    left = left_refs[0][0]
    for j in range(1, count // 2):
        left = jnp.where(step // 2 == j, left_refs[j][0], left)
    left = (left * n_row).astype(jnp.bfloat16)
    right = jnp.where(n_col > 0.0, arrived[:, :hidden] * n_col, 0.0)
    total = jnp.sum(right * right, axis=1, keepdims=True)
    scale = lax.rsqrt(total / right.shape[1] + stability_offset)
    low = jnp.dot(left, right.astype(jnp.bfloat16), preferred_element_type=jnp.float32)
    kept = c_ref[0].astype(jnp.float32)
    mom_ref[0] = (kept - (1.0 - momentum_decay) * low).astype(jnp.bfloat16)
    q_new = (right * scale).astype(jnp.bfloat16)
    upd = jnp.dot(left, q_new, preferred_element_type=jnp.float32) * multiplier
    upd_ref[0] = upd.astype(jnp.bfloat16)
    slot = where[1, base + step]

    @pl.when(slot < cap)
    def _():
        share = q_ref.shape[1]
        start = pl.multiple_of(where[2, 0] * share, share)
        own = jnp.where(n_col > 0.0, buf[:, pl.ds(start, share)] * n_col, 0.0) * scale
        q_ref[slot] = own.T.astype(jnp.bfloat16)


def last_call(where, base, combined, left, rights, outs, cap, share, multiplier):
    experts, rows, hidden = combined.shape
    count, pairs = len(rights) // 2, len(left)
    rank, width = rights[0].shape
    rank *= 2
    block = pl.BlockSpec((1, rows, hidden), lambda i, w: (w[0, base + i], 0, 0))
    anywhere = pl.BlockSpec(memory_space=pl.ANY)
    extra = [] if outs is None else [outs[2], outs[0], outs[1]]
    return pl.pallas_call(
        functools.partial(last_body, count, multiplier, cap, base, outs is None),
        grid_spec=pltpu.PrefetchScalarGridSpec(
            num_scalar_prefetch=1,
            grid=(count,),
            in_specs=[block]
            + [
                pl.BlockSpec((1, rows, rank), lambda i, w, j=j: (jnp.clip(i - 2 * j, 0, 1), 0, 0))
                for j in range(len(left))
            ]
            + [pl.BlockSpec(memory_space=pltpu.VMEM)] * len(rights)
            + ([] if outs is None else [fixed((cap, share, rank)), anywhere, anywhere]),
            out_specs=[block, block, fixed((cap, share, rank))],
            scratch_shapes=[pltpu.VMEM((rank, width), jnp.float32)],
        ),
        out_shape=[
            jax.ShapeDtypeStruct((experts, rows, hidden), jnp.bfloat16),
            jax.ShapeDtypeStruct((experts, rows, hidden), jnp.bfloat16),
            jax.ShapeDtypeStruct((cap, share, rank), jnp.bfloat16),
        ],
        input_output_aliases={} if outs is None else {3 + pairs + 2 * count: 0, 4 + pairs + 2 * count: 1},
        cost_estimate=pl.CostEstimate(
            flops=WEIGHT * count * 4 * rows * hidden * rank,
            bytes_accessed=count * 2 * (3 * rows + 2 * rank) * hidden,
            transcendentals=0,
        ),
        compiler_params=pltpu.CompilerParams(vmem_limit_bytes=GRANT),
        name="last",
    )(where, combined, *left, *rights, *extra)


def step(momentum, gradient, q_prev, owner_group, group_counts):
    groups = lax.axis_size("group")
    shard_count = lax.axis_size("shard")
    experts, block, _ = momentum.shape
    _, cap, share, rank = q_prev.shape
    assert experts == groups
    links = Links(groups, shard_count)
    near, orders = links.orders()

    names = in_order(links.levels())
    sets = [[n for n in names if n.bit_count() == i] for i in range(links.levels() + 1)]

    def distances(side):
        reach = lambda name, at: sum(bit for i, bit in enumerate(orders[at]) if name >> i & 1)
        return [
            reach(name, side ^ far) ^ (near if far else 0)
            for name in names
            for far in (0, 1)
        ]

    uppers = [r for r in range(groups) if not r & near]
    where, kept, sent = plan_call(
        owner_group, group_counts, q_prev, (distances(0), distances(1)), near, uppers
    )
    arrived = links.swap_group(sent, near)
    parts = [kept[i] + arrived[i] for i in range(len(uppers))]
    q_own = parts[0]
    for part, r in zip(parts[1:], uppers[1:]):
        q_own = q_own + links.swap_group(part, r)
    combined = add_call(momentum, gradient)
    q_own, combined = lax.optimization_barrier((q_own, combined))
    q_full = links.gather_shard(q_own)
    qs = [links.spread(part) for part in q_full]
    qs_far = [{n: links.swap_group(x, near) for n, x in part.items()} for part in qs]

    lefts, rights = {}, {}
    for i, name in enumerate(names):
        own_side, far_side = ([side[0][name], side[1][name]] for side in (qs, qs_far))
        if name == names[-1]:
            far_left, far = first_call(where, 2 * i + 1, combined, far_side, shard_count)
            left, kept = first_call(where, 2 * i, combined, own_side, shard_count)
            lefts[name] = jnp.concatenate([left, far_left], axis=0)
            outs = [kept[0], far[0]]
        else:
            pieces = [x for pair in zip(own_side, far_side) for x in pair]
            lefts[name], outs = first_call(where, 2 * i, combined, pieces, shard_count)
        rights[name] = [outs[0], links.swap_group(outs[1], near)]

    own = rights.pop(0)
    sums = []
    for i in (0, 1):
        rows = slice(i * rank // 2, (i + 1) * rank // 2)
        held = {name: [term[rows] for term in terms] for name, terms in rights.items()}
        parts = links.collect({0: [], **held}, i == 0)
        pieces = split_call(where, i, own, parts, shard_count)
        mine_sum = pieces[0].astype(jnp.float32)
        for d in range(1, shard_count):
            mine_sum = mine_sum + links.swap_shard(pieces[d], d).astype(jnp.float32)
        sums.append(mine_sum)
    mine_sum = jnp.concatenate(sums, axis=0)
    right_own = links.gather_shard(mine_sum.astype(jnp.bfloat16))
    full = [links.spread(part) for part in right_own]
    full_far = [{n: links.swap_group(x, near) for n, x in part.items()} for part in full]

    multiplier = math.sqrt(block * groups * shard_count / rank)
    outs = None
    for members in sets:
        pieces = [
            side[half][n] for half in (0, 1) for n in members for side in (full, full_far)
        ]
        base = 2 * names.index(members[0])
        left = [lefts[n] for n in members]
        outs = last_call(
            where, base, combined, left, pieces, outs, cap, share, multiplier
        )
    momentum_next, update, q_next = outs
    return momentum_next, update, q_next[None]


def in_order(levels):
    return sorted(range(1 << levels), key=lambda name: (name.bit_count(), -name))


def solution(mesh):
    return jax.shard_map(
        step,
        mesh=mesh,
        in_specs=(
            P(None, ("group", "shard"), None),
            P(None, ("group", "shard"), None),
            P("group", None, "shard", None),
            P(),
            P(),
        ),
        out_specs=(
            P(None, ("group", "shard"), None),
            P(None, ("group", "shard"), None),
            P("group", None, "shard", None),
        ),
        check_vma=False,
    )
```
